32 devices in a mesh: groups: 2 (over y), blk: 4 (over z), ulysses: 2 (over x), cfg: 2 (over core).
Axes of the slice: x: 2, y: 2, z: 4, core: 2. Of those that a mesh axis runs over, the one named last changes fastest.
Arguments:
- img_tokens: bfloat16 [2, 2, 512, 2432], P('cfg', 'groups', ('blk', 'ulysses')), parts along dimension 1, may hold values from -72 to 72
- text_tokens: bfloat16 [2, 2, 48, 2432], P('cfg', 'groups', ('blk', 'ulysses')), parts along dimension 1, may hold values from -6 to 6
- text_lengths: int32 [2, 2], P('cfg', 'groups'), parts along dimension 1, may hold values from 12 to 48
- timestep: int32 [2], P('groups'), parts along dimension 0, may hold values from 0 to 999
- pooled: float32 [2, 2, 2432], P(None, 'groups'), parts along dimension 1, may hold values from -6 to 6
- time_weight: bfloat16 [256, 2432], replicated, may hold values from -0.375 to 0.375
- time_second: bfloat16 [2432, 2432], P(None, ('blk', 'ulysses', 'cfg')), may hold values from -0.125 to 0.125
- mod_weight: bfloat16 [2432, 24320], P(None, ('blk', 'ulysses', 'cfg')), may hold values from -0.125 to 0.125
- proj_weight: bfloat16 [5, 2432, 2048], P(None, None, ('ulysses', 'cfg')), may hold values from -0.125 to 0.125
- out_weight: bfloat16 [2048, 2432], P(('ulysses', 'cfg')), may hold values from -0.125 to 0.125
- expand_weight: bfloat16 [2432, 7168], P('blk', ('ulysses', 'cfg')), may hold values from -0.125 to 0.125
- reduce_weight: bfloat16 [7168, 2432], P(('ulysses', 'cfg'), 'blk'), may hold values from -0.0625 to 0.0625
- qk_gain: float32 [3, 64], replicated, may hold values from 0.5 to 10
- final_weight: bfloat16 [2432, 64], replicated, may hold values from -0.125 to 0.125
Outputs:
- guided: float32 [2, 16, 16, 128], P('groups', None, ('blk', 'ulysses', 'cfg')), parts along dimension 0
The draws below stay inside these ranges and needn't reach their ends.
There are 2 independent parts, one for each index of `groups`. The reference program is written for one: setup_inputs(seed, part) draws one part's arguments, and reference() takes and returns one part's arrays. A program takes and returns all parts, laid end to end along the dimension named above; an argument that names none is the same for every part. Nothing has to cross between parts.
All inputs are finite; a program needn't handle non-finite values.
Results may differ from the reference program's by a relative error of at most 0.011.
The reference program's roundings to bfloat16 on the way count: a program that leaves them out, or rounds other values in their place, can miss the bound.
Values may be sent and summed in bfloat16 or wider, within the bound.
A program may use at most 192 MiB of HBM per device.

```python
import math
import jax
import jax.numpy as jnp
from jax import lax

D = 2432
HEADS = 32
HD = 64
LAT = 16
FREQ = 256
FF = 7168
PROMPTS = 1
IMG_DEV = 64
INNER = 2048
PATCH_OUT = 64
IMG = 512
TXT = 48
N_ULYSSES = 2
N_CFG = 2


def draw_img_tokens(key, part):
    base_key, row_key, col_key = jax.random.split(jax.random.fold_in(key, 11), 3)
    full_shape = (2, PROMPTS, IMG, D)
    base_draw = jnp.clip(jax.random.normal(base_key, full_shape, jnp.float32), -4.0, 4.0)
    row_top = math.log(4.0)
    row_scale = jnp.exp(jax.random.uniform(row_key, (2, PROMPTS, IMG, 1), jnp.float32, 0.0, row_top))
    col_scale = jnp.exp(jax.random.uniform(col_key, (1, 1, 1, D), jnp.float32, math.log(0.5), math.log(2.0)))
    return (base_draw * row_scale * col_scale).astype(jnp.bfloat16)


def draw_qk_gain(key, part):
    gain_key = jax.random.fold_in(key, 23)
    low_end = math.log(0.5)
    high_end = math.log(2.0)
    return jnp.exp(jax.random.uniform(gain_key, (3, HD), jnp.float32, low_end, high_end))


def shard_levels(key, shape, cuts, smallest, largest):
    def one(position, blocks):
        heights = jax.random.uniform(jax.random.fold_in(jax.random.fold_in(key, 6), position), (blocks,), jnp.float32, smallest / len(cuts), largest / len(cuts))
        return jnp.repeat(jnp.exp(heights), shape[position] // blocks).reshape((-1,) + (1,) * (len(shape) - position - 1))

    level = one(*cuts[0])
    for cut in cuts[1:]:
        level = level * one(*cut)
    return level


def normal_values(stream_key, dims, deviation, bound, shards=(), kind=jnp.bfloat16):
    factor_of = shard_levels(stream_key, dims, shards, -0.22, 0.18) if shards else 1.0
    result = jax.random.normal(stream_key, dims, jnp.float32) * deviation * factor_of
    return jnp.minimum(jnp.maximum(result, -bound), bound).astype(kind)


def setup_inputs(seed: int = 0, part: int = 0) -> dict:
    key_list = jax.random.split(jax.random.key(seed), 15)
    part_keys = jax.random.split(jax.random.fold_in(key_list[14], part), 15)
    img_tokens = draw_img_tokens(jax.random.fold_in(jax.random.fold_in(key_list[14], part), 71), part)
    text_tokens = normal_values(part_keys[1], (2, PROMPTS, TXT, D), 1.0, 6.0, ((0, 2), (2, 8)))
    text_lengths = jax.random.randint(part_keys[2], (2, PROMPTS), TXT // 4, TXT + 1).astype(jnp.int32)
    timestep = jax.random.randint(part_keys[3], (PROMPTS,), 0, 1000).astype(jnp.int32)
    pooled = normal_values(part_keys[4], (2, PROMPTS, D), 1.0, 6.0, (), jnp.float32)
    time_weight = normal_values(key_list[5], (FREQ, D), FREQ ** -0.5, 0.375)
    time_second = normal_values(key_list[6], (D, D), D ** -0.5, 0.125, ((1, 16),))
    mod_weight = normal_values(key_list[7], (D, 10 * D), D ** -0.5, 0.125, ((1, 16),))
    proj_weight = normal_values(key_list[8], (5, D, INNER), D ** -0.5, 0.125, ((2, 4),))
    out_weight = normal_values(key_list[9], (INNER, D), INNER ** -0.5, 0.125, ((0, 4),))
    expand_weight = normal_values(key_list[10], (D, FF), D ** -0.5, 0.125, ((0, 4), (1, 4)))
    reduce_weight = normal_values(key_list[11], (FF, D), FF ** -0.5, 0.0625, ((0, 4), (1, 4)))
    qk_gain = draw_qk_gain(jax.random.fold_in(key_list[14], 71), part)
    final_weight = normal_values(key_list[13], (D, PATCH_OUT), D ** -0.5, 0.125)
    return {"img_tokens": img_tokens, "text_tokens": text_tokens, "text_lengths": text_lengths, "timestep": timestep, "pooled": pooled, "time_weight": time_weight, "time_second": time_second, "mod_weight": mod_weight, "proj_weight": proj_weight, "out_weight": out_weight, "expand_weight": expand_weight, "reduce_weight": reduce_weight, "qk_gain": qk_gain, "final_weight": final_weight}


GUIDANCE = 3.5
LN_EPS = 1e-06
RMS_EPS = 1e-06
NEG_FILL = -1e+30

def sinusoid(timestep, feature_count):
    half_width = feature_count // 2
    frequency = jnp.exp(-math.log(10000.0) * jnp.arange(half_width, dtype=jnp.float32) / half_width)
    angles = timestep.astype(jnp.float32)[:, None] * frequency[None, :]
    return jnp.concatenate([jnp.cos(angles), jnp.sin(angles)], axis=1)

def layer_norm(values):
    average = lax.optimization_barrier(jnp.mean(values, axis=-1, keepdims=True))
    centred = values - average
    variance = lax.optimization_barrier(jnp.mean(centred * centred, axis=-1, keepdims=True))
    return centred * lax.rsqrt(variance + LN_EPS)

def modulate(values, shift, scale):
    return (layer_norm(values.astype(jnp.float32)) * (1.0 + scale) + shift).astype(jnp.bfloat16)

def rms_heads(values, gain):
    head_size = gain.shape[0]
    shaped = values.reshape(values.shape[:-1] + (values.shape[-1] // head_size, head_size))
    inverse = lax.rsqrt(lax.optimization_barrier(jnp.mean(shaped * shaped, axis=-1, keepdims=True)) + RMS_EPS)
    return (shaped * inverse * gain).reshape(values.shape).astype(jnp.bfloat16)

def finish(img_proj, txt_proj, gain_rows):
    img_set = jnp.stack([rms_heads(img_proj[0], gain_rows[0]), rms_heads(img_proj[1], gain_rows[1]), img_proj[2].astype(jnp.bfloat16)])
    txt_set = jnp.stack([rms_heads(txt_proj[0], gain_rows[2]), txt_proj[1].astype(jnp.bfloat16)])
    return (img_set, txt_set)

def head_attention(query_head, key_head, value_head, usable):
    scores = jnp.dot(query_head, key_head.T, preferred_element_type=jnp.float32) * (1.0 / math.sqrt(query_head.shape[1]))
    scores = jnp.where(usable[None, :], scores, NEG_FILL)
    row_max = lax.optimization_barrier(jnp.max(scores, axis=1, keepdims=True))
    weights = jnp.where(usable[None, :], jnp.exp(scores - row_max), 0.0)
    row_total = lax.optimization_barrier(jnp.sum(weights, axis=1, keepdims=True))
    mixed = jnp.dot(weights.astype(jnp.bfloat16), value_head, preferred_element_type=jnp.float32) / row_total
    return mixed.astype(jnp.bfloat16)

def feed_forward(feed_input, expand_weight, reduce_weight):
    feed_hidden = jax.nn.gelu(jnp.dot(feed_input, expand_weight, preferred_element_type=jnp.float32), approximate=True).astype(jnp.bfloat16)
    group_count = N_ULYSSES * N_CFG
    group_width = reduce_weight.shape[0] // group_count
    feed_out = jnp.zeros((feed_input.shape[0], reduce_weight.shape[1]), jnp.float32)
    for group in range(group_count):
        term = jnp.dot(feed_hidden[:, group * group_width:(group + 1) * group_width], reduce_weight[group * group_width:(group + 1) * group_width], preferred_element_type=jnp.float32)
        term = lax.optimization_barrier(term.astype(jnp.bfloat16))
        feed_out = feed_out + term.astype(jnp.float32)
    return feed_out

def one_branch(image_rows, text_rows, length, mod_rows, proj_weight, out_weight, expand_weight, reduce_weight, qk_gain, final_weight):
    h_img = modulate(image_rows, mod_rows[0], mod_rows[1])
    h_txt = modulate(text_rows, mod_rows[4], mod_rows[3])
    img_proj = jnp.stack([jnp.dot(h_img, proj_weight[j], preferred_element_type=jnp.float32) for j in range(3)])
    txt_proj = jnp.stack([jnp.dot(h_txt, proj_weight[j], preferred_element_type=jnp.float32) for j in (3, 4)])
    img_set, txt_set = finish(img_proj, txt_proj, qk_gain)
    key_rows = jnp.concatenate([img_set[1], txt_set[0]], axis=0)
    value_rows = jnp.concatenate([img_set[2], txt_set[1]], axis=0)
    usable = jnp.concatenate([jnp.ones((IMG,), dtype=bool), jnp.arange(TXT, dtype=jnp.int32) < length])
    query_stack = img_set[0].reshape(IMG, HEADS, HD).transpose(1, 0, 2)
    key_stack = key_rows.reshape(IMG + TXT, HEADS, HD).transpose(1, 0, 2)
    value_stack = value_rows.reshape(IMG + TXT, HEADS, HD).transpose(1, 0, 2)

    def per_head(triple):
        return head_attention(triple[0], triple[1], triple[2], usable)
    mixed = lax.map(per_head, (query_stack, key_stack, value_stack))
    mixed = mixed.transpose(1, 0, 2).reshape(IMG, INNER)
    grouped = mixed.reshape(IMG, N_ULYSSES, INNER // N_ULYSSES).astype(jnp.float32)
    weight_groups = out_weight.reshape(N_ULYSSES, INNER // N_ULYSSES, D).astype(jnp.float32)
    group_terms = jnp.einsum('igc,gcd->gid', grouped, weight_groups, precision=lax.Precision.HIGHEST)
    group_terms = lax.optimization_barrier(group_terms.astype(jnp.bfloat16))
    attended = lax.optimization_barrier(jnp.sum(group_terms.astype(jnp.float32), axis=0))
    residual = image_rows.astype(jnp.float32) + mod_rows[2] * attended
    feed_input = modulate(residual, mod_rows[7], mod_rows[8])
    feed_out = feed_forward(feed_input, expand_weight, reduce_weight)
    second_residual = residual + mod_rows[9] * feed_out
    final_rows = modulate(second_residual, mod_rows[6], mod_rows[5])
    noise = jnp.dot(final_rows, final_weight, preferred_element_type=jnp.float32)
    noise = noise.reshape(IMG // IMG_DEV, IMG_DEV, 2, 2, LAT).transpose(4, 0, 2, 1, 3)
    return noise.reshape(LAT, 2 * IMG // IMG_DEV, 2 * IMG_DEV)

def reference(img_tokens, text_tokens, text_lengths, timestep, pooled, time_weight, time_second, mod_weight, proj_weight, out_weight, expand_weight, reduce_weight, qk_gain, final_weight):
    sinusoid_rows = sinusoid(timestep, time_weight.shape[0]).astype(jnp.bfloat16)
    time_hidden = jax.nn.silu(jnp.dot(sinusoid_rows, time_weight, preferred_element_type=jnp.float32)).astype(jnp.bfloat16)
    time_embed = jnp.dot(time_hidden, time_second, preferred_element_type=jnp.float32)
    acted = jax.nn.silu(time_embed[None] + pooled).astype(jnp.bfloat16)
    modulation = jnp.dot(acted.reshape(2 * PROMPTS, D), mod_weight, preferred_element_type=jnp.float32)
    modulation = modulation.reshape(2, PROMPTS, 10, D)
    results = []
    for prompt in range(PROMPTS):
        noises = []
        for branch in range(2):
            noises.append(one_branch(img_tokens[branch, prompt], text_tokens[branch, prompt], text_lengths[branch, prompt], modulation[branch, prompt], proj_weight, out_weight, expand_weight, reduce_weight, qk_gain, final_weight))
        noise_cond = noises[0]
        noise_uncond = noises[1]
        results.append(noise_uncond + GUIDANCE * (noise_cond - noise_uncond))
    return jnp.stack(results)
```

```python
import functools
import math

import jax
import jax.numpy as jnp
from jax import lax
from jax.experimental import pallas as pl
from jax.experimental.pallas import tpu as pltpu
from jax.sharding import PartitionSpec as P

GUIDANCE = 3.5
LN_EPS = 1e-06
RMS_EPS = 1e-06
NEG_FILL = -1e30
MESH = pl.DeviceIdType.MESH


def from_partner(value, axis, stride):
    mask = 2**stride
    pairs = [(source, source ^ mask) for source in range(lax.axis_size(axis))]
    return lax.ppermute(value, axis, pairs)


def sinusoid(timestep, feature_count):
    half_width = feature_count // 2
    frequency = jnp.exp(-math.log(10000.0) * jnp.arange(half_width, dtype=jnp.float32) / half_width)
    angles = timestep.astype(jnp.float32)[:, None] * frequency[None, :]
    return jnp.concatenate([jnp.cos(angles), jnp.sin(angles)], axis=1)


def layer_norm(values):
    average = jnp.mean(values, axis=-1, keepdims=True)
    centred = values - average
    variance = jnp.mean(centred * centred, axis=-1, keepdims=True)
    return centred * lax.rsqrt(variance + LN_EPS)


def modulate(values, shift, scale):
    return (layer_norm(values.astype(jnp.float32)) * (1.0 + scale) + shift).astype(jnp.bfloat16)


def rms_heads(values, gain):
    head_size = gain.shape[0]
    shaped = values.reshape(values.shape[:-1] + (values.shape[-1] // head_size, head_size))
    inverse = lax.rsqrt(jnp.mean(shaped * shaped, axis=-1, keepdims=True) + RMS_EPS)
    return (shaped * inverse * gain).reshape(values.shape).astype(jnp.bfloat16)


def flat_position(axes):
    position = 0
    for axis in axes:
        position = position * lax.axis_size(axis) + lax.axis_index(axis)
    return position


def coordinates(position, axes):
    found = {}
    for axis in reversed(axes):
        size = lax.axis_size(axis)
        found[axis] = lax.rem(position, size)
        position = position // size
    return found


def count_of(axes):
    return math.prod(lax.axis_size(axis) for axis in axes)


def direct_kernel(axes, swap, x_ref, o_ref, send_sem, recv_sem, local_sem):
    count = count_of(axes)
    me = flat_position(axes)
    barrier = pltpu.get_barrier_semaphore()

    def greet(step, carry):
        peer = lax.rem(me + step, count)
        pl.semaphore_signal(
            barrier, inc=1, device_id=coordinates(peer, axes), device_id_type=MESH
        )
        return carry

    lax.fori_loop(1, count, greet, 0)
    own = pltpu.make_async_copy(x_ref.at[me] if swap else x_ref, o_ref.at[me], local_sem)
    own.start()
    pl.semaphore_wait(barrier, count - 1)

    def outgoing(step):
        peer = lax.rem(me + step, count)
        return pltpu.make_async_remote_copy(
            src_ref=x_ref.at[peer] if swap else x_ref,
            dst_ref=o_ref.at[me],
            send_sem=send_sem.at[step],
            recv_sem=recv_sem.at[step],
            device_id=coordinates(peer, axes),
            device_id_type=MESH,
        )

    def incoming(step):
        source = lax.rem(me - step + count, count)
        return pltpu.make_async_remote_copy(
            src_ref=x_ref.at[source] if swap else x_ref,
            dst_ref=o_ref.at[source],
            send_sem=send_sem.at[step],
            recv_sem=recv_sem.at[step],
            device_id=coordinates(source, axes),
            device_id_type=MESH,
        )

    def begin(step, carry):
        outgoing(step).start()
        return carry

    def finish(step, carry):
        incoming(step).wait_recv()
        outgoing(step).wait_send()
        return carry

    lax.fori_loop(1, count, begin, 0)
    lax.fori_loop(1, count, finish, 0)
    own.wait()


def direct(value, axes, swap, collective_id, name):
    count = count_of(axes)
    shape = value.shape if swap else (count,) + value.shape
    return pl.pallas_call(
        functools.partial(direct_kernel, axes, swap),
        out_shape=jax.ShapeDtypeStruct(shape, value.dtype),
        in_specs=[pl.BlockSpec(memory_space=pltpu.VMEM)],
        out_specs=pl.BlockSpec(memory_space=pltpu.VMEM),
        scratch_shapes=[
            pltpu.SemaphoreType.DMA((count,)),
            pltpu.SemaphoreType.DMA((count,)),
            pltpu.SemaphoreType.DMA,
        ],
        compiler_params=pltpu.CompilerParams(collective_id=collective_id, has_side_effects=True),
        cost_estimate=pl.CostEstimate(
            flops=0, bytes_accessed=4 * math.prod(shape) + 4000000, transcendentals=0
        ),
        name=name,
    )(value)


def quad_kernel(
    chunks, x_ref, o_ref, send_u, recv_u, send_c, recv_c, send_f, recv_f, local_sem
):
    size = lax.axis_size("ulysses")
    row = lax.axis_index("ulysses")
    core = lax.axis_index("cfg")
    me = row * 2 + core
    partner = {"ulysses": row, "cfg": 1 - core}
    barrier = pltpu.get_barrier_semaphore()
    for step in range(1, size):
        pl.semaphore_signal(
            barrier,
            inc=1,
            device_id={"ulysses": lax.rem(row + step, size), "cfg": core},
            device_id_type=MESH,
        )
    pl.semaphore_signal(barrier, inc=1, device_id=partner, device_id_type=MESH)
    own = pltpu.make_async_copy(x_ref, o_ref.at[me], local_sem)
    own.start()
    pl.semaphore_wait(barrier, size)

    def across(step, chunk):
        return pltpu.make_async_remote_copy(
            src_ref=x_ref.at[chunk],
            dst_ref=o_ref.at[me, chunk],
            send_sem=send_u.at[step, chunk],
            recv_sem=recv_u.at[step, chunk],
            device_id={"ulysses": lax.rem(row + step, size), "cfg": core},
            device_id_type=MESH,
        )

    def landed(step, chunk):
        source = lax.rem(row - step + size, size)
        return pltpu.make_async_remote_copy(
            src_ref=x_ref.at[chunk],
            dst_ref=o_ref.at[source * 2 + core, chunk],
            send_sem=send_u.at[step, chunk],
            recv_sem=recv_u.at[step, chunk],
            device_id={"ulysses": source, "cfg": core},
            device_id_type=MESH,
        )

    def forward(step, chunk, side):
        source = lax.rem(row - step + size, size)
        return pltpu.make_async_remote_copy(
            src_ref=o_ref.at[source * 2 + side, chunk],
            dst_ref=o_ref.at[source * 2 + side, chunk],
            send_sem=send_f.at[step, chunk],
            recv_sem=recv_f.at[step, chunk],
            device_id=partner,
            device_id_type=MESH,
        )

    def beside(slot):
        return pltpu.make_async_remote_copy(
            src_ref=x_ref,
            dst_ref=o_ref.at[slot],
            send_sem=send_c,
            recv_sem=recv_c,
            device_id=partner,
            device_id_type=MESH,
        )

    pairs = [(step, chunk) for chunk in range(chunks) for step in range(1, size)]
    for step, chunk in pairs:
        across(step, chunk).start()
    beside(me).start()
    for step, chunk in pairs:
        landed(step, chunk).wait_recv()
        forward(step, chunk, core).start()
    for step, chunk in pairs:
        across(step, chunk).wait_send()
        forward(step, chunk, core).wait_send()
        forward(step, chunk, 1 - core).wait_recv()
    beside(me).wait_send()
    beside(row * 2 + 1 - core).wait_recv()
    own.wait()


def quad_gather(value, collective_id, name):
    size = lax.axis_size("ulysses")
    chunks = value.shape[0]
    shape = (size * 2,) + value.shape
    grid_sem = pltpu.SemaphoreType.DMA((size, chunks))
    return pl.pallas_call(
        functools.partial(quad_kernel, chunks),
        out_shape=jax.ShapeDtypeStruct(shape, value.dtype),
        in_specs=[pl.BlockSpec(memory_space=pl.ANY)],
        out_specs=pl.BlockSpec(memory_space=pl.ANY),
        scratch_shapes=[
            grid_sem,
            grid_sem,
            pltpu.SemaphoreType.DMA,
            pltpu.SemaphoreType.DMA,
            grid_sem,
            grid_sem,
            pltpu.SemaphoreType.DMA,
        ],
        compiler_params=pltpu.CompilerParams(collective_id=collective_id, has_side_effects=True),
        cost_estimate=pl.CostEstimate(
            flops=0, bytes_accessed=8 * math.prod(shape) + 4000000, transcendentals=0
        ),
        name=name,
    )(value)


def ring_rows(piece, axis):
    size = lax.axis_size(axis)
    me = lax.axis_index(axis)
    rows = piece.shape[0]
    up = [(source, (source + 1) % size) for source in range(size)]
    down = [(source, (source - 1) % size) for source in range(size)]
    whole = jnp.zeros((size * rows,) + piece.shape[1:], piece.dtype)

    def place(whole, part, owner, offset):
        return lax.dynamic_update_slice_in_dim(whole, part, owner * rows + offset, 0)

    whole = place(whole, piece, me, 0)
    upward = downward = piece
    for step in range(1, (size - 1) // 2 + 1):
        upward = lax.ppermute(upward, axis, up)
        downward = lax.ppermute(downward, axis, down)
        whole = place(whole, upward, lax.rem(me - step + size, size), 0)
        whole = place(whole, downward, lax.rem(me + step, size), 0)
    if size % 2 == 0:
        half = rows // 2 if size > 2 else rows
        far = lax.rem(me + size // 2, size)
        whole = place(whole, lax.ppermute(upward[:half], axis, up), far, 0)
        if half < rows:
            whole = place(whole, lax.ppermute(downward[half:], axis, down), far, half)
    return whole


def body(
    img_tokens,
    text_tokens,
    text_lengths,
    timestep,
    pooled,
    time_weight,
    time_second,
    mod_weight,
    proj_weight,
    out_weight,
    expand_weight,
    reduce_weight,
    qk_gain,
    final_weight,
):
    model_width = img_tokens.shape[3]
    prompts = img_tokens.shape[1]
    head_size = qk_gain.shape[1]
    branches = pooled.shape[0]
    branch = lax.axis_index("cfg")
    everyone = ("blk", "ulysses", "cfg")
    near = ("ulysses", "cfg")
    blocks = lax.axis_size("blk")
    sides = lax.axis_size("ulysses")
    expand_full = ring_rows(expand_weight, "blk")
    sinusoid_rows = sinusoid(timestep, time_weight.shape[0]).astype(jnp.bfloat16)
    time_hidden = jax.nn.silu(
        jnp.dot(sinusoid_rows, time_weight, preferred_element_type=jnp.float32)
    ).astype(jnp.bfloat16)
    time_part = jnp.dot(time_hidden, time_second, preferred_element_type=jnp.float32)
    time_width = time_part.shape[1]
    first = direct(
        jnp.concatenate([time_part, text_lengths[0][:, None].astype(jnp.float32)], axis=1),
        everyone,
        False,
        0,
        "gather_time",
    )
    time_embed = first[:, :, :time_width].transpose(1, 0, 2).reshape(prompts, -1)
    lengths = first[:branches, :, time_width].astype(jnp.int32)
    acted = jax.nn.silu(time_embed[None] + pooled).astype(jnp.bfloat16)
    mod_part = jnp.einsum("bpd,dc->bpc", acted, mod_weight, preferred_element_type=jnp.float32)
    mod_all = direct(mod_part, everyone, False, 1, "gather_mod")
    own_mod = lax.dynamic_index_in_dim(mod_all, branch, 1, keepdims=False)
    own_mod = own_mod.transpose(1, 0, 2).reshape(prompts, 10, model_width)
    image_rows = img_tokens[0]
    text_rows = text_tokens[0]
    token_count = image_rows.shape[1]
    slot_count = text_rows.shape[1]
    h_img = modulate(image_rows, own_mod[:, 0:1], own_mod[:, 1:2])
    h_txt = modulate(text_rows, own_mod[:, 4:5], own_mod[:, 3:4])
    rows_all = quad_gather(
        jnp.concatenate([h_img, h_txt], axis=1), 2, "gather_rows"
    )
    rows_all = rows_all.reshape(sides, branches, prompts, token_count + slot_count, model_width)
    rows_img = rows_all[:, :, :, :token_count]
    rows_txt = rows_all[:, :, :, token_count:]
    img_proj = jnp.einsum(
        "ubprd,jdc->jubprc", rows_img, proj_weight[0:3], preferred_element_type=jnp.float32
    )
    txt_proj = jnp.einsum(
        "ubprd,jdc->jubprc", rows_txt, proj_weight[3:5], preferred_element_type=jnp.float32
    )
    queries = rms_heads(img_proj[0], qk_gain[0])
    img_kv = jnp.stack([rms_heads(img_proj[1], qk_gain[1]), img_proj[2].astype(jnp.bfloat16)])
    txt_kv = jnp.stack([rms_heads(txt_proj[0], qk_gain[2]), txt_proj[1].astype(jnp.bfloat16)])
    inner_local = queries.shape[-1]
    head_count = inner_local // head_size
    own_kv = jnp.concatenate([img_kv, txt_kv], axis=4)
    all_kv = lax.all_gather(own_kv, "blk", axis=0, tiled=False)
    span = token_count + slot_count
    all_kv = all_kv.reshape(
        blocks, 2, sides, branches, prompts, span, head_count, head_size
    )
    query_heads = queries.reshape(sides, branches, prompts, token_count, head_count, head_size)
    scale = 1.0 / math.sqrt(head_size)
    scores = (
        jnp.einsum(
            "ubpqhd,zvbpkhd->bphuqzvk",
            query_heads,
            all_kv[:, 0],
            preferred_element_type=jnp.float32,
        )
        * scale
    )
    place = jnp.arange(span, dtype=jnp.int32) - token_count
    slot = (
        jnp.arange(blocks * sides, dtype=jnp.int32).reshape(blocks, sides, 1) * slot_count + place
    )
    allowed = (place < 0) | (slot < lengths[:, :, None, None, None])
    allowed = allowed[:, :, None, None, None]
    scores = jnp.where(allowed, scores, NEG_FILL)
    largest = jnp.max(scores, axis=(5, 6, 7), keepdims=True)
    weights = jnp.where(allowed, jnp.exp(scores - largest), 0.0)
    denominator = jnp.sum(weights, axis=(5, 6, 7))
    mixed = jnp.einsum(
        "bphuqzvk,zvbpkhd->bphuqd",
        weights.astype(jnp.bfloat16),
        all_kv[:, 1],
        preferred_element_type=jnp.float32,
    )
    mixed = (mixed / denominator[..., None]).astype(jnp.bfloat16)
    mixed_rows = mixed.transpose(3, 0, 1, 4, 2, 5).reshape(-1, inner_local)
    out_terms = jnp.dot(mixed_rows, out_weight, preferred_element_type=jnp.float32)
    out_terms = out_terms.astype(jnp.bfloat16).reshape(
        sides * branches, prompts * token_count, model_width
    )
    out_terms = direct(out_terms, near, True, 3, "swap_out")
    attended = jnp.sum(out_terms.astype(jnp.float32), axis=0)
    attended = attended.reshape(prompts, token_count, model_width)
    residual = image_rows.astype(jnp.float32) + own_mod[:, 2:3] * attended
    feed_input = modulate(residual, own_mod[:, 7:8], own_mod[:, 8:9]).reshape(
        prompts * token_count, model_width
    )
    feed_blocks = lax.all_gather(feed_input, "blk", axis=0, tiled=False)
    feed_all = quad_gather(feed_blocks, 4, "gather_feed").reshape(-1, model_width)
    pre_active = jnp.dot(feed_all, expand_full, preferred_element_type=jnp.float32)
    feed_hidden = jax.nn.gelu(pre_active, approximate=True).astype(jnp.bfloat16)
    feed_terms = jnp.dot(feed_hidden, reduce_weight, preferred_element_type=jnp.float32)
    feed_terms = feed_terms.astype(jnp.bfloat16).reshape(
        sides * branches * blocks, prompts * token_count, -1
    )
    feed_terms = direct(feed_terms, ("ulysses", "cfg", "blk"), True, 5, "swap_feed")
    feed_terms = feed_terms.reshape(sides * branches, blocks, prompts * token_count, -1)
    feed_out = jnp.sum(feed_terms.astype(jnp.float32), axis=0).transpose(1, 0, 2)
    second_residual = residual + own_mod[:, 9:10] * feed_out.reshape(
        prompts, token_count, model_width
    )
    final_rows = modulate(second_residual, own_mod[:, 6:7], own_mod[:, 5:6])
    noise = jnp.einsum("prd,dc->prc", final_rows, final_weight, preferred_element_type=jnp.float32)
    latent_channels = final_weight.shape[1] // 4
    noise_own = noise.reshape(prompts, token_count, 2, 2, latent_channels).transpose(0, 4, 2, 1, 3)
    noise_own = noise_own.reshape(prompts, latent_channels, 2, 2 * token_count)
    kept_row = lax.dynamic_slice_in_dim(noise_own, branch, 1, 2)
    sent_row = lax.dynamic_slice_in_dim(noise_own, 1 - branch, 1, 2)
    noise_pair = from_partner(sent_row, "cfg", 0)
    noise_cond = jnp.where(branch == 0, kept_row, noise_pair)
    noise_uncond = jnp.where(branch == 0, noise_pair, kept_row)
    return noise_uncond + GUIDANCE * (noise_cond - noise_uncond)


def solution(mesh):
    in_specs = (
        P("cfg", "groups", ("blk", "ulysses"), None),
        P("cfg", "groups", ("blk", "ulysses"), None),
        P("cfg", "groups"),
        P("groups"),
        P(None, "groups", None),
        P(),
        P(None, ("blk", "ulysses", "cfg")),
        P(None, ("blk", "ulysses", "cfg")),
        P(None, None, ("ulysses", "cfg")),
        P(("ulysses", "cfg"), None),
        P("blk", ("ulysses", "cfg")),
        P(("ulysses", "cfg"), "blk"),
        P(),
        P(),
    )
    out_specs = P("groups", None, ("blk", "ulysses", "cfg"), None)
    return jax.shard_map(body, mesh=mesh, in_specs=in_specs, out_specs=out_specs, check_vma=False)
```

```python
import functools
import math

import jax
import jax.numpy as jnp
from jax import lax
from jax.experimental import pallas as pl
from jax.experimental.pallas import tpu as pltpu
from jax.sharding import PartitionSpec as P


GUIDANCE = 3.5
LN_EPS = 1e-06
RMS_EPS = 1e-06
NEG_FILL = -1e30
MESH = pl.DeviceIdType.MESH


def from_partner(value, axis, stride):
    mask = 2**stride
    pairs = [(source, source ^ mask) for source in range(lax.axis_size(axis))]
    return lax.ppermute(value, axis, pairs)


def sinusoid(timestep, feature_count):
    half_width = feature_count // 2
    frequency = jnp.exp(-math.log(10000.0) * jnp.arange(half_width, dtype=jnp.float32) / half_width)
    angles = timestep.astype(jnp.float32)[:, None] * frequency[None, :]
    return jnp.concatenate([jnp.cos(angles), jnp.sin(angles)], axis=1)


def layer_norm(values):
    average = jnp.mean(values, axis=-1, keepdims=True)
    centred = values - average
    variance = jnp.mean(centred * centred, axis=-1, keepdims=True)
    return centred * lax.rsqrt(variance + LN_EPS)


def modulate(values, shift, scale):
    return (layer_norm(values.astype(jnp.float32)) * (1.0 + scale) + shift).astype(jnp.bfloat16)


def rms_heads(values, gain):
    head_size = gain.shape[0]
    shaped = values.reshape(values.shape[:-1] + (values.shape[-1] // head_size, head_size))
    inverse = lax.rsqrt(jnp.mean(shaped * shaped, axis=-1, keepdims=True) + RMS_EPS)
    return (shaped * inverse * gain).reshape(values.shape).astype(jnp.bfloat16)


def flat_position(axes):
    position = 0
    for axis in axes:
        position = position * lax.axis_size(axis) + lax.axis_index(axis)
    return position


def coordinates(position, axes):
    found = {}
    for axis in reversed(axes):
        size = lax.axis_size(axis)
        found[axis] = lax.rem(position, size)
        position = position // size
    return found


def count_of(axes):
    return math.prod(lax.axis_size(axis) for axis in axes)


def direct_kernel(axes, swap, x_ref, o_ref, send_sem, recv_sem, local_sem):
    count = count_of(axes)
    me = flat_position(axes)
    barrier = pltpu.get_barrier_semaphore()

    def greet(step, carry):
        peer = lax.rem(me + step, count)
        pl.semaphore_signal(
            barrier, inc=1, device_id=coordinates(peer, axes), device_id_type=MESH
        )
        return carry

    lax.fori_loop(1, count, greet, 0)
    own = pltpu.make_async_copy(x_ref.at[me] if swap else x_ref, o_ref.at[me], local_sem)
    own.start()
    pl.semaphore_wait(barrier, count - 1)

    def outgoing(step):
        peer = lax.rem(me + step, count)
        return pltpu.make_async_remote_copy(
            src_ref=x_ref.at[peer] if swap else x_ref,
            dst_ref=o_ref.at[me],
            send_sem=send_sem.at[step],
            recv_sem=recv_sem.at[step],
            device_id=coordinates(peer, axes),
            device_id_type=MESH,
        )

    def incoming(step):
        source = lax.rem(me - step + count, count)
        return pltpu.make_async_remote_copy(
            src_ref=x_ref.at[source] if swap else x_ref,
            dst_ref=o_ref.at[source],
            send_sem=send_sem.at[step],
            recv_sem=recv_sem.at[step],
            device_id=coordinates(source, axes),
            device_id_type=MESH,
        )

    def begin(step, carry):
        outgoing(step).start()
        return carry

    def finish(step, carry):
        incoming(step).wait_recv()
        outgoing(step).wait_send()
        return carry

    lax.fori_loop(1, count, begin, 0)
    lax.fori_loop(1, count, finish, 0)
    own.wait()


def direct(value, axes, swap, collective_id):
    count = count_of(axes)
    shape = value.shape if swap else (count,) + value.shape
    return pl.pallas_call(
        functools.partial(direct_kernel, axes, swap),
        out_shape=jax.ShapeDtypeStruct(shape, value.dtype),
        in_specs=[pl.BlockSpec(memory_space=pltpu.VMEM)],
        out_specs=pl.BlockSpec(memory_space=pltpu.VMEM),
        scratch_shapes=[
            pltpu.SemaphoreType.DMA((count,)),
            pltpu.SemaphoreType.DMA((count,)),
            pltpu.SemaphoreType.DMA,
        ],
        compiler_params=pltpu.CompilerParams(collective_id=collective_id, has_side_effects=True),
        cost_estimate=pl.CostEstimate(
            flops=0, bytes_accessed=4 * math.prod(shape) + 4000000, transcendentals=0
        ),
    )(value)


def quad_kernel(
    chunks, x_ref, o_ref, send_u, recv_u, send_c, recv_c, send_f, recv_f, local_sem
):
    size = lax.axis_size("ulysses")
    row = lax.axis_index("ulysses")
    core = lax.axis_index("cfg")
    me = row * 2 + core
    partner = {"ulysses": row, "cfg": 1 - core}
    barrier = pltpu.get_barrier_semaphore()
    for step in range(1, size):
        pl.semaphore_signal(
            barrier,
            inc=1,
            device_id={"ulysses": lax.rem(row + step, size), "cfg": core},
            device_id_type=MESH,
        )
    pl.semaphore_signal(barrier, inc=1, device_id=partner, device_id_type=MESH)
    own = pltpu.make_async_copy(x_ref, o_ref.at[me], local_sem)
    own.start()
    pl.semaphore_wait(barrier, size)

    def across(step, chunk):
        return pltpu.make_async_remote_copy(
            src_ref=x_ref.at[chunk],
            dst_ref=o_ref.at[me, chunk],
            send_sem=send_u.at[step, chunk],
            recv_sem=recv_u.at[step, chunk],
            device_id={"ulysses": lax.rem(row + step, size), "cfg": core},
            device_id_type=MESH,
        )

    def landed(step, chunk):
        source = lax.rem(row - step + size, size)
        return pltpu.make_async_remote_copy(
            src_ref=x_ref.at[chunk],
            dst_ref=o_ref.at[source * 2 + core, chunk],
            send_sem=send_u.at[step, chunk],
            recv_sem=recv_u.at[step, chunk],
            device_id={"ulysses": source, "cfg": core},
            device_id_type=MESH,
        )

    def forward(step, chunk, side):
        source = lax.rem(row - step + size, size)
        return pltpu.make_async_remote_copy(
            src_ref=o_ref.at[source * 2 + side, chunk],
            dst_ref=o_ref.at[source * 2 + side, chunk],
            send_sem=send_f.at[step, chunk],
            recv_sem=recv_f.at[step, chunk],
            device_id=partner,
            device_id_type=MESH,
        )

    def beside(slot):
        return pltpu.make_async_remote_copy(
            src_ref=x_ref,
            dst_ref=o_ref.at[slot],
            send_sem=send_c,
            recv_sem=recv_c,
            device_id=partner,
            device_id_type=MESH,
        )

    pairs = [(step, chunk) for chunk in range(chunks) for step in range(1, size)]
    for step, chunk in pairs:
        across(step, chunk).start()
    beside(me).start()
    for step, chunk in pairs:
        landed(step, chunk).wait_recv()
        forward(step, chunk, core).start()
    for step, chunk in pairs:
        across(step, chunk).wait_send()
        forward(step, chunk, core).wait_send()
        forward(step, chunk, 1 - core).wait_recv()
    beside(me).wait_send()
    beside(row * 2 + 1 - core).wait_recv()
    own.wait()


def quad_gather(value, collective_id):
    size = lax.axis_size("ulysses")
    chunks = value.shape[0]
    shape = (size * 2,) + value.shape
    grid_sem = pltpu.SemaphoreType.DMA((size, chunks))
    return pl.pallas_call(
        functools.partial(quad_kernel, chunks),
        out_shape=jax.ShapeDtypeStruct(shape, value.dtype),
        in_specs=[pl.BlockSpec(memory_space=pl.ANY)],
        out_specs=pl.BlockSpec(memory_space=pl.ANY),
        scratch_shapes=[
            grid_sem,
            grid_sem,
            pltpu.SemaphoreType.DMA,
            pltpu.SemaphoreType.DMA,
            grid_sem,
            grid_sem,
            pltpu.SemaphoreType.DMA,
        ],
        compiler_params=pltpu.CompilerParams(collective_id=collective_id, has_side_effects=True),
        cost_estimate=pl.CostEstimate(
            flops=0, bytes_accessed=8 * math.prod(shape) + 4000000, transcendentals=0
        ),
    )(value)


def ring_kernel(axis, spread, x_ref, o_ref, hop_s, hop_r, x_s, x_r, c_s, c_r, f_s, f_r, local_sem):
    size = lax.axis_size(axis)
    me = lax.axis_index(axis)
    last = size // 2
    halved = size % 2 == 0
    sides = lax.axis_size("ulysses") if spread else 1
    row = lax.axis_index("ulysses")
    core = lax.axis_index("cfg")
    partner = {"ulysses": row, "cfg": 1 - core}
    base = o_ref.at[row * 2 + core] if spread else o_ref

    def at(offset):
        return lax.rem(me + offset + size, size)

    def aside(step):
        return {"ulysses": lax.rem(row + step, sides), "cfg": core}

    barrier = pltpu.get_barrier_semaphore()
    for way in (1, -1):
        pl.semaphore_signal(barrier, inc=1, device_id={axis: at(way)}, device_id_type=MESH)
    if spread:
        for step in range(1, sides):
            pl.semaphore_signal(barrier, inc=1, device_id=aside(step), device_id_type=MESH)
        pl.semaphore_signal(barrier, inc=1, device_id=partner, device_id_type=MESH)
    own = pltpu.make_async_copy(x_ref, base.at[me], local_sem)
    own.start()
    pl.semaphore_wait(barrier, 2 + (sides if spread else 0))

    def part(ref, way, step):
        if halved and step == last:
            return ref.at[0 if way == 1 else 1]
        return ref

    def hop(way, step):
        slot = at(-way * (step - 1))
        source = x_ref if step == 1 else base.at[slot]
        return pltpu.make_async_remote_copy(
            src_ref=part(source, way, step),
            dst_ref=part(base.at[slot], way, step),
            send_sem=hop_s.at[(way + 1) // 2, step],
            recv_sem=hop_r.at[(way + 1) // 2, step],
            device_id={axis: at(way)},
            device_id_type=MESH,
        )

    def hop_in(way, step):
        slot = base.at[at(-way * step)]
        return pltpu.make_async_remote_copy(
            src_ref=part(slot, way, step),
            dst_ref=part(slot, way, step),
            send_sem=hop_s.at[(way + 1) // 2, step],
            recv_sem=hop_r.at[(way + 1) // 2, step],
            device_id={axis: at(-way)},
            device_id_type=MESH,
        )

    def send(order, offset, step):
        slot = at(offset)
        return pltpu.make_async_remote_copy(
            src_ref=x_ref if order == 0 else base.at[slot],
            dst_ref=base.at[slot],
            send_sem=x_s.at[order, step] if step else c_s.at[order],
            recv_sem=x_r.at[order, step] if step else c_r.at[order],
            device_id=aside(step) if step else partner,
            device_id_type=MESH,
        )

    def across_in(order, offset, step):
        source = lax.rem(row - step + sides, sides)
        block = o_ref.at[source * 2 + core, at(offset)]
        return pltpu.make_async_remote_copy(
            src_ref=block,
            dst_ref=block,
            send_sem=x_s.at[order, step],
            recv_sem=x_r.at[order, step],
            device_id=aside(step),
            device_id_type=MESH,
        )

    def forward(order, offset, step, side):
        source = lax.rem(row - step + sides, sides)
        block = o_ref.at[source * 2 + side, at(offset)]
        return pltpu.make_async_remote_copy(
            src_ref=block,
            dst_ref=block,
            send_sem=f_s.at[order, step],
            recv_sem=f_r.at[order, step],
            device_id=partner,
            device_id_type=MESH,
        )

    def beside_in(order, offset):
        block = o_ref.at[row * 2 + 1 - core, at(offset)]
        return pltpu.make_async_remote_copy(
            src_ref=block,
            dst_ref=block,
            send_sem=c_s.at[order],
            recv_sem=c_r.at[order],
            device_id=partner,
            device_id_type=MESH,
        )

    steps = last
    offsets = [0]
    for way in (1, -1):
        hop(way, 1).start()
    sent = []

    def pass_on(order, offset):
        if spread:
            for step in list(range(1, sides)) + [0]:
                send(order, offset, step).start()
            sent.append((order, offset))

    def relay(order, offset):
        for step in range(1, sides):
            across_in(order, offset, step).wait_recv()
            forward(order, offset, step, core).start()

    pass_on(0, 0)
    relayed = 0
    for step in range(1, steps + 1):
        final = halved and step == last
        for way in (1, -1):
            hop_in(way, step).wait_recv()
            if step < steps:
                hop(way, step + 1).start()
            if not final:
                offsets.append(-way * step)
                pass_on(len(offsets) - 1, offsets[-1])
        if final:
            offsets.append(step)
            pass_on(len(offsets) - 1, step)
        if spread:
            while relayed < len(offsets) - 2:
                relay(relayed, offsets[relayed])
                relayed += 1
    if spread:
        while relayed < len(offsets):
            relay(relayed, offsets[relayed])
            relayed += 1
    for step in range(1, steps + 1):
        for way in (1, -1):
            hop(way, step).wait_send()
    for order, offset in sent:
        for step in range(sides):
            send(order, offset, step).wait_send()
        for step in range(1, sides):
            forward(order, offset, step, core).wait_send()
            forward(order, offset, step, 1 - core).wait_recv()
        beside_in(order, offset).wait_recv()
    own.wait()


def ring_gather(value, axis, spread, collective_id):
    size = lax.axis_size(axis)
    sides = lax.axis_size("ulysses")
    shape = (size,) + value.shape
    if spread:
        shape = (sides * 2,) + shape
    space = pl.ANY if spread else pltpu.VMEM
    hops = pltpu.SemaphoreType.DMA((2, size // 2 + 1))
    across = pltpu.SemaphoreType.DMA((size, sides))
    beside = pltpu.SemaphoreType.DMA((size,))
    return pl.pallas_call(
        functools.partial(ring_kernel, axis, spread),
        out_shape=jax.ShapeDtypeStruct(shape, value.dtype),
        in_specs=[pl.BlockSpec(memory_space=space)],
        out_specs=pl.BlockSpec(memory_space=space),
        scratch_shapes=[hops, hops, across, across, beside, beside, across, across]
        + [pltpu.SemaphoreType.DMA],
        compiler_params=pltpu.CompilerParams(collective_id=collective_id, has_side_effects=True),
        cost_estimate=pl.CostEstimate(
            flops=0, bytes_accessed=8 * math.prod(shape) + 4000000, transcendentals=0
        ),
    )(value)


def ring_rows(piece, axis):
    size = lax.axis_size(axis)
    me = lax.axis_index(axis)
    rows = piece.shape[0]
    up = [(source, (source + 1) % size) for source in range(size)]
    down = [(source, (source - 1) % size) for source in range(size)]
    whole = jnp.zeros((size * rows,) + piece.shape[1:], piece.dtype)

    def place(whole, part, owner, offset):
        return lax.dynamic_update_slice_in_dim(whole, part, owner * rows + offset, 0)

    whole = place(whole, piece, me, 0)
    upward = downward = piece
    for step in range(1, (size - 1) // 2 + 1):
        upward = lax.ppermute(upward, axis, up)
        downward = lax.ppermute(downward, axis, down)
        whole = place(whole, upward, lax.rem(me - step + size, size), 0)
        whole = place(whole, downward, lax.rem(me + step, size), 0)
    if size % 2 == 0:
        half = rows // 2 if size > 2 else rows
        far = lax.rem(me + size // 2, size)
        upward = lax.ppermute(upward[:half], axis, up)
        whole = place(whole, upward, far, 0)
        if half < rows:
            downward = lax.ppermute(downward[half:], axis, down)
            whole = place(whole, downward, far, half)
    return whole


def body(
    img_tokens,
    text_tokens,
    text_lengths,
    timestep,
    pooled,
    time_weight,
    time_second,
    mod_weight,
    proj_weight,
    out_weight,
    expand_weight,
    reduce_weight,
    qk_gain,
    final_weight,
):
    model_width = img_tokens.shape[3]
    prompts = img_tokens.shape[1]
    head_size = qk_gain.shape[1]
    branches = pooled.shape[0]
    branch = lax.axis_index("cfg")
    everyone = ("blk", "ulysses", "cfg")
    near = ("ulysses", "cfg")
    blocks = lax.axis_size("blk")
    sides = lax.axis_size("ulysses")
    expand_full = ring_rows(expand_weight, "blk")
    sinusoid_rows = sinusoid(timestep, time_weight.shape[0]).astype(jnp.bfloat16)
    time_hidden = jax.nn.silu(
        jnp.dot(sinusoid_rows, time_weight, preferred_element_type=jnp.float32)
    ).astype(jnp.bfloat16)
    time_part = jnp.dot(time_hidden, time_second, preferred_element_type=jnp.float32)
    time_width = time_part.shape[1]
    first = direct(
        jnp.concatenate([time_part, text_lengths[0][:, None].astype(jnp.float32)], axis=1),
        everyone,
        False,
        0,
    )
    time_embed = first[:, :, :time_width].transpose(1, 0, 2).reshape(prompts, -1)
    lengths = first[:branches, :, time_width].astype(jnp.int32)
    acted = jax.nn.silu(time_embed[None] + pooled).astype(jnp.bfloat16)
    mod_part = jnp.einsum("bpd,dc->bpc", acted, mod_weight, preferred_element_type=jnp.float32)
    mod_all = direct(mod_part, everyone, False, 1)
    own_mod = lax.dynamic_index_in_dim(mod_all, branch, 1, keepdims=False)
    own_mod = own_mod.transpose(1, 0, 2).reshape(prompts, 10, model_width)
    image_rows = img_tokens[0]
    text_rows = text_tokens[0]
    token_count = image_rows.shape[1]
    slot_count = text_rows.shape[1]
    h_img = modulate(image_rows, own_mod[:, 0:1], own_mod[:, 1:2])
    h_txt = modulate(text_rows, own_mod[:, 4:5], own_mod[:, 3:4])
    rows_own = jnp.concatenate([h_img, h_txt], axis=1)
    rows_all = quad_gather(rows_own, 2)
    rows_all = rows_all.reshape(sides, branches, prompts, token_count + slot_count, model_width)
    rows_img = rows_all[:, :, :, :token_count]
    rows_txt = rows_all[:, :, :, token_count:]
    img_proj = jnp.einsum(
        "ubprd,jdc->jubprc", rows_img, proj_weight[0:3], preferred_element_type=jnp.float32
    )
    txt_proj = jnp.einsum(
        "ubprd,jdc->jubprc", rows_txt, proj_weight[3:5], preferred_element_type=jnp.float32
    )
    queries = rms_heads(img_proj[0], qk_gain[0])
    img_kv = jnp.stack([rms_heads(img_proj[1], qk_gain[1]), img_proj[2].astype(jnp.bfloat16)])
    txt_kv = jnp.stack([rms_heads(txt_proj[0], qk_gain[2]), txt_proj[1].astype(jnp.bfloat16)])
    inner_local = queries.shape[-1]
    head_count = inner_local // head_size
    own_kv = jnp.concatenate([img_kv, txt_kv], axis=4)
    all_kv = ring_gather(own_kv, "blk", False, 6)
    span = token_count + slot_count
    all_kv = all_kv.reshape(
        blocks, 2, sides, branches, prompts, span, head_count, head_size
    )
    query_heads = queries.reshape(sides, branches, prompts, token_count, head_count, head_size)
    scale = 1.0 / math.sqrt(head_size)
    scores = (
        jnp.einsum(
            "ubpqhd,zvbpkhd->bphuqzvk",
            query_heads,
            all_kv[:, 0],
            preferred_element_type=jnp.float32,
        )
        * scale
    )
    place = jnp.arange(span, dtype=jnp.int32) - token_count
    slot = (
        jnp.arange(blocks * sides, dtype=jnp.int32).reshape(blocks, sides, 1) * slot_count + place
    )
    allowed = (place < 0) | (slot < lengths[:, :, None, None, None])
    allowed = allowed[:, :, None, None, None]
    scores = jnp.where(allowed, scores, NEG_FILL)
    largest = jnp.max(scores, axis=(5, 6, 7), keepdims=True)
    weights = jnp.where(allowed, jnp.exp(scores - largest), 0.0)
    denominator = jnp.sum(weights, axis=(5, 6, 7))
    mixed = jnp.einsum(
        "bphuqzvk,zvbpkhd->bphuqd",
        weights.astype(jnp.bfloat16),
        all_kv[:, 1],
        preferred_element_type=jnp.float32,
    )
    mixed = (mixed / denominator[..., None]).astype(jnp.bfloat16)
    mixed_rows = mixed.transpose(3, 0, 1, 4, 2, 5).reshape(-1, inner_local)
    out_terms = jnp.dot(mixed_rows, out_weight, preferred_element_type=jnp.float32)
    out_terms = out_terms.astype(jnp.bfloat16).reshape(
        sides * branches, prompts * token_count, model_width
    )
    out_terms = direct(out_terms, near, True, 3)
    attended = jnp.sum(out_terms.astype(jnp.float32), axis=0)
    attended = attended.reshape(prompts, token_count, model_width)
    residual = image_rows.astype(jnp.float32) + own_mod[:, 2:3] * attended
    feed_input = modulate(residual, own_mod[:, 7:8], own_mod[:, 8:9]).reshape(
        prompts * token_count, model_width
    )
    feed_halves = feed_input.reshape(2, -1, model_width)
    feed_all = ring_gather(feed_halves, "blk", True, 4).reshape(-1, model_width)
    pre_active = jnp.dot(feed_all, expand_full, preferred_element_type=jnp.float32)
    feed_hidden = jax.nn.gelu(pre_active, approximate=True).astype(jnp.bfloat16)
    feed_terms = jnp.dot(feed_hidden, reduce_weight, preferred_element_type=jnp.float32)
    feed_terms = feed_terms.astype(jnp.bfloat16).reshape(
        sides * branches * blocks, prompts * token_count, -1
    )
    feed_terms = direct(feed_terms, ("ulysses", "cfg", "blk"), True, 5)
    feed_terms = feed_terms.reshape(sides * branches, blocks, prompts * token_count, -1)
    feed_out = jnp.sum(feed_terms.astype(jnp.float32), axis=0).transpose(1, 0, 2)
    second_residual = residual + own_mod[:, 9:10] * feed_out.reshape(
        prompts, token_count, model_width
    )
    final_rows = modulate(second_residual, own_mod[:, 6:7], own_mod[:, 5:6])
    noise = jnp.einsum("prd,dc->prc", final_rows, final_weight, preferred_element_type=jnp.float32)
    latent_channels = final_weight.shape[1] // 4
    noise_own = noise.reshape(prompts, token_count, 2, 2, latent_channels).transpose(0, 4, 2, 1, 3)
    noise_own = noise_own.reshape(prompts, latent_channels, 2, 2 * token_count)
    kept_row = lax.dynamic_slice_in_dim(noise_own, branch, 1, 2)
    sent_row = lax.dynamic_slice_in_dim(noise_own, 1 - branch, 1, 2)
    noise_pair = from_partner(sent_row, "cfg", 0)
    noise_cond = jnp.where(branch == 0, kept_row, noise_pair)
    noise_uncond = jnp.where(branch == 0, noise_pair, kept_row)
    return noise_uncond + GUIDANCE * (noise_cond - noise_uncond)


def solution(mesh):
    in_specs = (
        P("cfg", "groups", ("blk", "ulysses"), None),
        P("cfg", "groups", ("blk", "ulysses"), None),
        P("cfg", "groups"),
        P("groups"),
        P(None, "groups", None),
        P(),
        P(None, ("blk", "ulysses", "cfg")),
        P(None, ("blk", "ulysses", "cfg")),
        P(None, None, ("ulysses", "cfg")),
        P(("ulysses", "cfg"), None),
        P("blk", ("ulysses", "cfg")),
        P(("ulysses", "cfg"), "blk"),
        P(),
        P(),
    )
    out_specs = P("groups", None, ("blk", "ulysses", "cfg"), None)


    return jax.shard_map(body, mesh=mesh, in_specs=in_specs, out_specs=out_specs, check_vma=False)
```

```python
import functools
import math

import jax
import jax.numpy as jnp
from jax import lax
from jax.experimental import pallas as pl
from jax.experimental.pallas import tpu as pltpu
from jax.sharding import PartitionSpec as P


GUIDANCE = 3.5
LN_EPS = 1e-06
RMS_EPS = 1e-06
NEG_FILL = -1e30
MESH = pl.DeviceIdType.MESH


def from_partner(value, axis, stride):
    mask = 2**stride
    pairs = [(source, source ^ mask) for source in range(lax.axis_size(axis))]
    return lax.ppermute(value, axis, pairs)


def sinusoid(timestep, feature_count):
    half_width = feature_count // 2
    frequency = jnp.exp(-math.log(10000.0) * jnp.arange(half_width, dtype=jnp.float32) / half_width)
    angles = timestep.astype(jnp.float32)[:, None] * frequency[None, :]
    return jnp.concatenate([jnp.cos(angles), jnp.sin(angles)], axis=1)


def layer_norm(values):
    average = jnp.mean(values, axis=-1, keepdims=True)
    centred = values - average
    variance = jnp.mean(centred * centred, axis=-1, keepdims=True)
    return centred * lax.rsqrt(variance + LN_EPS)


def modulate(values, shift, scale):
    return (layer_norm(values.astype(jnp.float32)) * (1.0 + scale) + shift).astype(jnp.bfloat16)


def rms_heads(values, gain):
    head_size = gain.shape[0]
    width = values.shape[-1]
    head_of = jnp.arange(width, dtype=jnp.int32) // head_size
    same_head = (head_of[:, None] == head_of[None, :]).astype(jnp.float32) / head_size
    mean_square = jnp.dot(
        values * values,
        same_head,
        precision=lax.Precision.HIGHEST,
        preferred_element_type=jnp.float32,
    )
    gains = jnp.tile(gain, width // head_size)
    return (values * lax.rsqrt(mean_square + RMS_EPS) * gains).astype(jnp.bfloat16)


def attention_kernel(head_size, q_ref, kv_ref, allowed_ref, o_ref):
    sides, batch, rows, width = q_ref.shape
    blocks, _, _, span, _ = kv_ref.shape
    lanes = 2 * head_size
    scale = 1.0 / math.sqrt(head_size)
    low = lax.broadcasted_iota(jnp.int32, (1, lanes), 1) < head_size
    for item in range(batch):
        allowed = allowed_ref[item] > 0.0
        for first in range(0, width, lanes):
            here = slice(first, first + lanes)
            queries = q_ref[:, item, :, here].reshape(sides * rows, lanes)
            keys = kv_ref[:, 0, item, :, here].reshape(blocks * span, lanes)
            values = kv_ref[:, 1, item, :, here].reshape(blocks * span, lanes)
            mixed = []
            for chosen in (low, jnp.logical_not(low)):
                one_head = jnp.where(chosen, queries, jnp.zeros_like(queries))
                scores = (
                    lax.dot_general(
                        one_head,
                        keys,
                        (((1,), (1,)), ((), ())),
                        preferred_element_type=jnp.float32,
                    )
                    * scale
                )
                scores = jnp.where(allowed, scores, NEG_FILL)
                largest = jnp.max(scores, axis=1, keepdims=True)
                weights = jnp.where(allowed, jnp.exp(scores - largest), 0.0)
                denominator = jnp.sum(weights, axis=1, keepdims=True)
                update = jnp.dot(
                    weights.astype(jnp.bfloat16), values, preferred_element_type=jnp.float32
                )
                mixed.append(update / denominator)
            both = jnp.where(low, mixed[0], mixed[1]).astype(jnp.bfloat16)
            o_ref[:, item, :, here] = both.reshape(sides, rows, lanes)


def attention(queries, all_kv, allowed, head_size):
    sides, batch, rows, width = queries.shape
    keys = all_kv.shape[0] * all_kv.shape[3]
    products = batch * sides * rows * keys * width
    return pl.pallas_call(
        functools.partial(attention_kernel, head_size),
        out_shape=jax.ShapeDtypeStruct(queries.shape, jnp.bfloat16),
        in_specs=[pl.BlockSpec(memory_space=pltpu.VMEM)] * 3,
        out_specs=pl.BlockSpec(memory_space=pltpu.VMEM),
        cost_estimate=pl.CostEstimate(
            flops=8 * products,
            bytes_accessed=4 * batch * keys * width + 4 * batch * sides * rows * width,
            transcendentals=products // head_size,
        ),
        name="attention",
    )(queries, all_kv, allowed)


def reduce_kernel(axes, x_ref, o_ref, got, mine, core_s, core_r, far_s, far_r):
    count = count_of(axes)
    me = flat_position(axes)
    core = lax.axis_index("cfg")
    partner = {"cfg": 1 - core}
    barrier = pltpu.get_barrier_semaphore()
    pl.semaphore_signal(barrier, inc=1, device_id=partner, device_id_type=MESH)

    def target(step):
        return lax.rem(me + step, count)

    def greet(step, carry):
        pl.semaphore_signal(
            barrier, inc=1, device_id=coordinates(target(step), axes), device_id_type=MESH
        )
        return carry

    lax.fori_loop(1, count, greet, 0)
    pl.semaphore_wait(barrier, count)

    def beside(step):
        slot = target(step)
        return pltpu.make_async_remote_copy(
            src_ref=x_ref.at[1 - core, slot],
            dst_ref=got.at[slot],
            send_sem=core_s.at[slot],
            recv_sem=core_r.at[slot],
            device_id=partner,
            device_id_type=MESH,
        )

    def far(step):
        slot = target(step)
        return pltpu.make_async_remote_copy(
            src_ref=mine.at[slot],
            dst_ref=o_ref.at[me],
            send_sem=far_s.at[step],
            recv_sem=far_r.at[step],
            device_id=coordinates(slot, axes),
            device_id_type=MESH,
        )

    def far_in(step):
        source = lax.rem(me - step + count, count)
        return pltpu.make_async_remote_copy(
            src_ref=mine.at[source],
            dst_ref=o_ref.at[source],
            send_sem=far_s.at[step],
            recv_sem=far_r.at[step],
            device_id=coordinates(source, axes),
            device_id_type=MESH,
        )

    def total(slot):
        beside_sum = x_ref[core, slot].astype(jnp.float32) + got[slot].astype(jnp.float32)
        return beside_sum.astype(jnp.bfloat16)

    def begin(step, carry):
        beside(step).start()
        return carry

    def send(step, carry):
        beside(step).wait_recv()
        mine[target(step)] = total(target(step))
        far(step).start()
        return carry

    def finish(step, carry):
        far_in(step).wait_recv()
        far(step).wait_send()
        beside(step).wait_send()
        return carry

    lax.fori_loop(1, count + 1, begin, 0)
    lax.fori_loop(1, count, send, 0)
    beside(0).wait_recv()
    o_ref[me] = total(me)
    lax.fori_loop(1, count, finish, 0)
    beside(0).wait_send()


def reduce_cores(value, axes, collective_id):
    shape = value.shape[1:]
    count = shape[0]
    sems = pltpu.SemaphoreType.DMA((count,))
    return pl.pallas_call(
        functools.partial(reduce_kernel, axes),
        out_shape=jax.ShapeDtypeStruct(shape, value.dtype),
        in_specs=[pl.BlockSpec(memory_space=pltpu.VMEM)],
        out_specs=pl.BlockSpec(memory_space=pltpu.VMEM),
        scratch_shapes=[
            pltpu.VMEM(shape, value.dtype),
            pltpu.VMEM(shape, value.dtype),
            sems,
            sems,
            sems,
            sems,
        ],
        compiler_params=pltpu.CompilerParams(collective_id=collective_id, has_side_effects=True),
        cost_estimate=pl.CostEstimate(
            flops=0, bytes_accessed=8 * math.prod(shape) + 4000000, transcendentals=0
        ),
    )(value)


def flat_position(axes):
    position = 0
    for axis in axes:
        position = position * lax.axis_size(axis) + lax.axis_index(axis)
    return position


def coordinates(position, axes):
    found = {}
    for axis in reversed(axes):
        size = lax.axis_size(axis)
        found[axis] = lax.rem(position, size)
        position = position // size
    return found


def count_of(axes):
    return math.prod(lax.axis_size(axis) for axis in axes)


def direct_kernel(axes, swap, x_ref, o_ref, send_sem, recv_sem, local_sem):
    count = count_of(axes)
    me = flat_position(axes)
    barrier = pltpu.get_barrier_semaphore()

    def greet(step, carry):
        peer = lax.rem(me + step, count)
        pl.semaphore_signal(
            barrier, inc=1, device_id=coordinates(peer, axes), device_id_type=MESH
        )
        return carry

    lax.fori_loop(1, count, greet, 0)
    own = pltpu.make_async_copy(x_ref.at[me] if swap else x_ref, o_ref.at[me], local_sem)
    own.start()
    pl.semaphore_wait(barrier, count - 1)

    def outgoing(step):
        peer = lax.rem(me + step, count)
        return pltpu.make_async_remote_copy(
            src_ref=x_ref.at[peer] if swap else x_ref,
            dst_ref=o_ref.at[me],
            send_sem=send_sem.at[step],
            recv_sem=recv_sem.at[step],
            device_id=coordinates(peer, axes),
            device_id_type=MESH,
        )

    def incoming(step):
        source = lax.rem(me - step + count, count)
        return pltpu.make_async_remote_copy(
            src_ref=x_ref.at[source] if swap else x_ref,
            dst_ref=o_ref.at[source],
            send_sem=send_sem.at[step],
            recv_sem=recv_sem.at[step],
            device_id=coordinates(source, axes),
            device_id_type=MESH,
        )

    def begin(step, carry):
        outgoing(step).start()
        return carry

    def finish(step, carry):
        incoming(step).wait_recv()
        outgoing(step).wait_send()
        return carry

    lax.fori_loop(1, count, begin, 0)
    lax.fori_loop(1, count, finish, 0)
    own.wait()


def direct(value, axes, swap, collective_id):
    count = count_of(axes)
    shape = value.shape if swap else (count,) + value.shape
    return pl.pallas_call(
        functools.partial(direct_kernel, axes, swap),
        out_shape=jax.ShapeDtypeStruct(shape, value.dtype),
        in_specs=[pl.BlockSpec(memory_space=pltpu.VMEM)],
        out_specs=pl.BlockSpec(memory_space=pltpu.VMEM),
        scratch_shapes=[
            pltpu.SemaphoreType.DMA((count,)),
            pltpu.SemaphoreType.DMA((count,)),
            pltpu.SemaphoreType.DMA,
        ],
        compiler_params=pltpu.CompilerParams(collective_id=collective_id, has_side_effects=True),
        cost_estimate=pl.CostEstimate(
            flops=0, bytes_accessed=4 * math.prod(shape) + 4000000, transcendentals=0
        ),
    )(value)


def quad_kernel(
    chunks, x_ref, o_ref, send_u, recv_u, send_c, recv_c, send_f, recv_f, local_sem
):
    size = lax.axis_size("ulysses")
    row = lax.axis_index("ulysses")
    core = lax.axis_index("cfg")
    me = row * 2 + core
    partner = {"ulysses": row, "cfg": 1 - core}
    barrier = pltpu.get_barrier_semaphore()
    for step in range(1, size):
        pl.semaphore_signal(
            barrier,
            inc=1,
            device_id={"ulysses": lax.rem(row + step, size), "cfg": core},
            device_id_type=MESH,
        )
    pl.semaphore_signal(barrier, inc=1, device_id=partner, device_id_type=MESH)
    own = pltpu.make_async_copy(x_ref, o_ref.at[me], local_sem)
    own.start()
    pl.semaphore_wait(barrier, size)

    def across(step, chunk):
        return pltpu.make_async_remote_copy(
            src_ref=x_ref.at[chunk],
            dst_ref=o_ref.at[me, chunk],
            send_sem=send_u.at[step, chunk],
            recv_sem=recv_u.at[step, chunk],
            device_id={"ulysses": lax.rem(row + step, size), "cfg": core},
            device_id_type=MESH,
        )

    def landed(step, chunk):
        source = lax.rem(row - step + size, size)
        return pltpu.make_async_remote_copy(
            src_ref=x_ref.at[chunk],
            dst_ref=o_ref.at[source * 2 + core, chunk],
            send_sem=send_u.at[step, chunk],
            recv_sem=recv_u.at[step, chunk],
            device_id={"ulysses": source, "cfg": core},
            device_id_type=MESH,
        )

    def forward(step, chunk, side):
        source = lax.rem(row - step + size, size)
        return pltpu.make_async_remote_copy(
            src_ref=o_ref.at[source * 2 + side, chunk],
            dst_ref=o_ref.at[source * 2 + side, chunk],
            send_sem=send_f.at[step, chunk],
            recv_sem=recv_f.at[step, chunk],
            device_id=partner,
            device_id_type=MESH,
        )

    def beside(slot):
        return pltpu.make_async_remote_copy(
            src_ref=x_ref,
            dst_ref=o_ref.at[slot],
            send_sem=send_c,
            recv_sem=recv_c,
            device_id=partner,
            device_id_type=MESH,
        )

    pairs = [(step, chunk) for chunk in range(chunks) for step in range(1, size)]
    for step, chunk in pairs:
        across(step, chunk).start()
    beside(me).start()
    for step, chunk in pairs:
        landed(step, chunk).wait_recv()
        forward(step, chunk, core).start()
    for step, chunk in pairs:
        across(step, chunk).wait_send()
        forward(step, chunk, core).wait_send()
        forward(step, chunk, 1 - core).wait_recv()
    beside(me).wait_send()
    beside(row * 2 + 1 - core).wait_recv()
    own.wait()


def quad_gather(value, collective_id):
    size = lax.axis_size("ulysses")
    chunks = value.shape[0]
    shape = (size * 2,) + value.shape
    grid_sem = pltpu.SemaphoreType.DMA((size, chunks))
    return pl.pallas_call(
        functools.partial(quad_kernel, chunks),
        out_shape=jax.ShapeDtypeStruct(shape, value.dtype),
        in_specs=[pl.BlockSpec(memory_space=pl.ANY)],
        out_specs=pl.BlockSpec(memory_space=pl.ANY),
        scratch_shapes=[
            grid_sem,
            grid_sem,
            pltpu.SemaphoreType.DMA,
            pltpu.SemaphoreType.DMA,
            grid_sem,
            grid_sem,
            pltpu.SemaphoreType.DMA,
        ],
        compiler_params=pltpu.CompilerParams(collective_id=collective_id, has_side_effects=True),
        cost_estimate=pl.CostEstimate(
            flops=0, bytes_accessed=8 * math.prod(shape) + 4000000, transcendentals=0
        ),
    )(value)


def ring_kernel(axis, spread, x_ref, o_ref, hop_s, hop_r, x_s, x_r, c_s, c_r, f_s, f_r, local_sem):
    size = lax.axis_size(axis)
    me = lax.axis_index(axis)
    last = size // 2
    halved = size % 2 == 0
    sides = lax.axis_size("ulysses") if spread else 1
    row = lax.axis_index("ulysses")
    core = lax.axis_index("cfg")
    partner = {"ulysses": row, "cfg": 1 - core}
    base = o_ref.at[row * 2 + core] if spread else o_ref

    def at(offset):
        return lax.rem(me + offset + size, size)

    def aside(step):
        return {"ulysses": lax.rem(row + step, sides), "cfg": core}

    barrier = pltpu.get_barrier_semaphore()
    for way in (1, -1):
        pl.semaphore_signal(barrier, inc=1, device_id={axis: at(way)}, device_id_type=MESH)
    if spread:
        for step in range(1, sides):
            pl.semaphore_signal(barrier, inc=1, device_id=aside(step), device_id_type=MESH)
        pl.semaphore_signal(barrier, inc=1, device_id=partner, device_id_type=MESH)
    own = pltpu.make_async_copy(x_ref, base.at[me], local_sem)
    own.start()
    pl.semaphore_wait(barrier, 2 + (sides if spread else 0))

    def part(ref, way, step):
        if halved and step == last:
            return ref.at[0 if way == 1 else 1]
        return ref

    def hop(way, step):
        slot = at(-way * (step - 1))
        source = x_ref if step == 1 else base.at[slot]
        return pltpu.make_async_remote_copy(
            src_ref=part(source, way, step),
            dst_ref=part(base.at[slot], way, step),
            send_sem=hop_s.at[(way + 1) // 2, step],
            recv_sem=hop_r.at[(way + 1) // 2, step],
            device_id={axis: at(way)},
            device_id_type=MESH,
        )

    def hop_in(way, step):
        slot = base.at[at(-way * step)]
        return pltpu.make_async_remote_copy(
            src_ref=part(slot, way, step),
            dst_ref=part(slot, way, step),
            send_sem=hop_s.at[(way + 1) // 2, step],
            recv_sem=hop_r.at[(way + 1) // 2, step],
            device_id={axis: at(-way)},
            device_id_type=MESH,
        )

    def send(order, offset, step):
        slot = at(offset)
        return pltpu.make_async_remote_copy(
            src_ref=x_ref if order == 0 else base.at[slot],
            dst_ref=base.at[slot],
            send_sem=x_s.at[order, step] if step else c_s.at[order],
            recv_sem=x_r.at[order, step] if step else c_r.at[order],
            device_id=aside(step) if step else partner,
            device_id_type=MESH,
        )

    def across_in(order, offset, step):
        source = lax.rem(row - step + sides, sides)
        block = o_ref.at[source * 2 + core, at(offset)]
        return pltpu.make_async_remote_copy(
            src_ref=block,
            dst_ref=block,
            send_sem=x_s.at[order, step],
            recv_sem=x_r.at[order, step],
            device_id=aside(step),
            device_id_type=MESH,
        )

    def forward(order, offset, step, side):
        source = lax.rem(row - step + sides, sides)
        block = o_ref.at[source * 2 + side, at(offset)]
        return pltpu.make_async_remote_copy(
            src_ref=block,
            dst_ref=block,
            send_sem=f_s.at[order, step],
            recv_sem=f_r.at[order, step],
            device_id=partner,
            device_id_type=MESH,
        )

    def beside_in(order, offset):
        block = o_ref.at[row * 2 + 1 - core, at(offset)]
        return pltpu.make_async_remote_copy(
            src_ref=block,
            dst_ref=block,
            send_sem=c_s.at[order],
            recv_sem=c_r.at[order],
            device_id=partner,
            device_id_type=MESH,
        )

    steps = last
    offsets = [0]
    for way in (1, -1):
        hop(way, 1).start()
    sent = []

    def pass_on(order, offset):
        if spread:
            for step in list(range(1, sides)) + [0]:
                send(order, offset, step).start()
            sent.append((order, offset))

    def relay(order, offset):
        for step in range(1, sides):
            across_in(order, offset, step).wait_recv()
            forward(order, offset, step, core).start()

    pass_on(0, 0)
    relayed = 0
    for step in range(1, steps + 1):
        final = halved and step == last
        for way in (1, -1):
            hop_in(way, step).wait_recv()
            if step < steps:
                hop(way, step + 1).start()
            if not final:
                offsets.append(-way * step)
                pass_on(len(offsets) - 1, offsets[-1])
        if final:
            offsets.append(step)
            pass_on(len(offsets) - 1, step)
        if spread:
            while relayed < len(offsets) - 2:
                relay(relayed, offsets[relayed])
                relayed += 1
    if spread:
        while relayed < len(offsets):
            relay(relayed, offsets[relayed])
            relayed += 1
    for step in range(1, steps + 1):
        for way in (1, -1):
            hop(way, step).wait_send()
    for order, offset in sent:
        for step in range(sides):
            send(order, offset, step).wait_send()
        for step in range(1, sides):
            forward(order, offset, step, core).wait_send()
            forward(order, offset, step, 1 - core).wait_recv()
        beside_in(order, offset).wait_recv()
    own.wait()


def ring_gather(value, axis, spread, collective_id):
    size = lax.axis_size(axis)
    sides = lax.axis_size("ulysses")
    shape = (size,) + value.shape
    if spread:
        shape = (sides * 2,) + shape
    space = pl.ANY if spread else pltpu.VMEM
    hops = pltpu.SemaphoreType.DMA((2, size // 2 + 1))
    across = pltpu.SemaphoreType.DMA((size, sides))
    beside = pltpu.SemaphoreType.DMA((size,))
    return pl.pallas_call(
        functools.partial(ring_kernel, axis, spread),
        out_shape=jax.ShapeDtypeStruct(shape, value.dtype),
        in_specs=[pl.BlockSpec(memory_space=space)],
        out_specs=pl.BlockSpec(memory_space=space),
        scratch_shapes=[hops, hops, across, across, beside, beside, across, across]
        + [pltpu.SemaphoreType.DMA],
        compiler_params=pltpu.CompilerParams(collective_id=collective_id, has_side_effects=True),
        cost_estimate=pl.CostEstimate(
            flops=0, bytes_accessed=8 * math.prod(shape) + 4000000, transcendentals=0
        ),
    )(value)


class WeightRing:
    def __init__(self, piece, axis, across):
        self.axis, self.across = axis, across
        self.size = lax.axis_size(axis)
        self.parts = lax.axis_size(across)
        self.me = lax.axis_index(axis)
        self.part = lax.axis_index(across)
        self.rows = piece.shape[0]
        self.share = self.rows // self.parts
        self.up = [(source, (source + 1) % self.size) for source in range(self.size)]
        self.down = [(source, (source - 1) % self.size) for source in range(self.size)]
        whole = jnp.zeros((self.size * self.rows,) + piece.shape[1:], piece.dtype)
        self.whole = lax.dynamic_update_slice_in_dim(whole, piece, self.me * self.rows, 0)
        own = lax.dynamic_slice_in_dim(piece, self.part * self.share, self.share, 0)
        self.upward = self.downward = own

    def place(self, block, owner, offset):
        for step in range(self.parts):
            if step:
                pairs = [(part, (part + step) % self.parts) for part in range(self.parts)]
                moved = lax.ppermute(block, self.across, pairs)
            else:
                moved = block
            origin = lax.rem(self.part - step + self.parts, self.parts)
            start = owner * self.rows + origin * self.share + offset
            self.whole = lax.dynamic_update_slice_in_dim(self.whole, moved, start, 0)

    def hop(self, step, after):
        size, me = self.size, self.me
        self.upward, self.downward, after = lax.optimization_barrier(
            (self.upward, self.downward, after)
        )
        if step <= (size - 1) // 2:
            self.upward = lax.ppermute(self.upward, self.axis, self.up)
            self.downward = lax.ppermute(self.downward, self.axis, self.down)
            self.place(self.upward, lax.rem(me - step + size, size), 0)
            self.place(self.downward, lax.rem(me + step, size), 0)
        else:
            half = self.share // 2
            far = lax.rem(me + step, size)
            low = lax.ppermute(self.upward[:half], self.axis, self.up)
            high = lax.ppermute(self.downward[half:], self.axis, self.down)
            self.place(jnp.concatenate([low, high], axis=0), far, 0)
        return after


def body(
    img_tokens,
    text_tokens,
    text_lengths,
    timestep,
    pooled,
    time_weight,
    time_second,
    mod_weight,
    proj_weight,
    out_weight,
    expand_weight,
    reduce_weight,
    qk_gain,
    final_weight,
):
    model_width = img_tokens.shape[3]
    prompts = img_tokens.shape[1]
    branches = pooled.shape[0]
    branch = lax.axis_index("cfg")
    everyone = ("blk", "ulysses", "cfg")
    blocks = lax.axis_size("blk")
    sides = lax.axis_size("ulysses")
    ring = WeightRing(expand_weight, "blk", "groups")
    sinusoid_rows = sinusoid(timestep, time_weight.shape[0]).astype(jnp.bfloat16)
    time_hidden = jax.nn.silu(
        jnp.dot(sinusoid_rows, time_weight, preferred_element_type=jnp.float32)
    ).astype(jnp.bfloat16)
    time_part = jnp.dot(time_hidden, time_second, preferred_element_type=jnp.float32)
    time_width = time_part.shape[1]
    first = direct(
        jnp.concatenate([time_part, text_lengths[0][:, None].astype(jnp.float32)], axis=1),
        everyone,
        False,
        0,
    )
    time_embed = first[:, :, :time_width].transpose(1, 0, 2).reshape(prompts, -1)
    lengths = first[:branches, :, time_width].astype(jnp.int32)
    acted = jax.nn.silu(time_embed[None] + pooled).astype(jnp.bfloat16)
    mod_part = jnp.einsum("bpd,dc->bpc", acted, mod_weight, preferred_element_type=jnp.float32)
    mod_all = direct(mod_part, everyone, False, 1)
    mod_all = ring.hop(1, mod_all)
    own_mod = lax.dynamic_index_in_dim(mod_all, branch, 1, keepdims=False)
    own_mod = own_mod.transpose(1, 0, 2).reshape(prompts, 10, model_width)
    image_rows = img_tokens[0]
    text_rows = text_tokens[0]
    token_count = image_rows.shape[1]
    slot_count = text_rows.shape[1]
    h_img = modulate(image_rows, own_mod[:, 0:1], own_mod[:, 1:2])
    h_txt = modulate(text_rows, own_mod[:, 4:5], own_mod[:, 3:4])
    rows_own = jnp.concatenate([h_img, h_txt], axis=1)
    rows_all = quad_gather(rows_own, 2)
    rows_all = rows_all.reshape(sides, branches, prompts, token_count + slot_count, model_width)
    rows_img = rows_all[:, :, :, :token_count]
    rows_txt = rows_all[:, :, :, token_count:]
    img_proj = jnp.einsum(
        "ubprd,jdc->jubprc", rows_img, proj_weight[0:3], preferred_element_type=jnp.float32
    )
    txt_proj = jnp.einsum(
        "ubprd,jdc->jubprc", rows_txt, proj_weight[3:5], preferred_element_type=jnp.float32
    )
    batch = branches * prompts
    inner_local = img_proj.shape[-1]
    queries = rms_heads(img_proj[0], qk_gain[0]).reshape(sides, batch, token_count, inner_local)

    def by_item(keys, values):
        pair = jnp.stack([keys, values]).reshape(2, sides, batch, -1, inner_local)
        return pair.transpose(0, 2, 1, 3, 4).reshape(2, batch, -1, inner_local)

    img_kv = by_item(rms_heads(img_proj[1], qk_gain[1]), img_proj[2].astype(jnp.bfloat16))
    txt_kv = by_item(rms_heads(txt_proj[0], qk_gain[2]), txt_proj[1].astype(jnp.bfloat16))
    img_span = img_kv.shape[2]
    txt_span = txt_kv.shape[2]
    padding = -txt_span % 16
    own_kv = jnp.concatenate(
        [img_kv, jnp.pad(txt_kv, ((0, 0), (0, 0), (0, padding), (0, 0)))], axis=2
    )
    all_kv = ring_gather(own_kv, "blk", False, 6)
    for step in range(2, blocks // 2 + 1):
        all_kv = ring.hop(step, all_kv)
    place = jnp.arange(img_span + txt_span + padding, dtype=jnp.int32) - img_span
    slot = jnp.arange(blocks, dtype=jnp.int32)[:, None] * txt_span + place
    live = (slot < lengths.reshape(batch, 1, 1)) & (place < txt_span)
    allowed = ((place < 0) | live).astype(jnp.float32).reshape(batch, 1, -1)
    mixed = attention(queries, all_kv, allowed, qk_gain.shape[1])
    out_terms = jnp.dot(
        mixed.reshape(-1, inner_local), out_weight, preferred_element_type=jnp.float32
    )
    out_terms = out_terms.astype(jnp.bfloat16).reshape(
        sides, branches, prompts * token_count, model_width
    )
    out_terms = out_terms.transpose(1, 0, 2, 3)
    out_terms = reduce_cores(out_terms, ("ulysses",), 3)
    attended = jnp.sum(out_terms.astype(jnp.float32), axis=0)
    attended = attended.reshape(prompts, token_count, model_width)
    residual = image_rows.astype(jnp.float32) + own_mod[:, 2:3] * attended
    feed_input = modulate(residual, own_mod[:, 7:8], own_mod[:, 8:9]).reshape(
        prompts * token_count, model_width
    )
    feed_halves = feed_input.reshape(2, -1, model_width)
    feed_all = ring_gather(feed_halves, "blk", True, 4)
    feed_all = feed_all.reshape(-1, model_width)
    pre_active = jnp.dot(feed_all, ring.whole, preferred_element_type=jnp.float32)
    feed_hidden = jax.nn.gelu(pre_active, approximate=True).astype(jnp.bfloat16)
    feed_terms = jnp.dot(feed_hidden, reduce_weight, preferred_element_type=jnp.float32)
    feed_terms = feed_terms.astype(jnp.bfloat16).reshape(
        sides, branches, blocks, prompts * token_count, -1
    )
    feed_terms = feed_terms.transpose(1, 0, 2, 3, 4).reshape(
        branches, sides * blocks, prompts * token_count, -1
    )
    feed_terms = reduce_cores(feed_terms, ("ulysses", "blk"), 5)
    feed_terms = feed_terms.reshape(sides, blocks, prompts * token_count, -1)
    feed_out = jnp.sum(feed_terms.astype(jnp.float32), axis=0).transpose(1, 0, 2)
    second_residual = residual + own_mod[:, 9:10] * feed_out.reshape(
        prompts, token_count, model_width
    )
    final_rows = modulate(second_residual, own_mod[:, 6:7], own_mod[:, 5:6])
    noise = jnp.einsum("prd,dc->prc", final_rows, final_weight, preferred_element_type=jnp.float32)
    latent_channels = final_weight.shape[1] // 4
    noise_own = noise.reshape(prompts, token_count, 2, 2, latent_channels).transpose(0, 4, 2, 1, 3)
    noise_own = noise_own.reshape(prompts, latent_channels, 2, 2 * token_count)
    kept_row = lax.dynamic_slice_in_dim(noise_own, branch, 1, 2)
    sent_row = lax.dynamic_slice_in_dim(noise_own, 1 - branch, 1, 2)
    noise_pair = from_partner(sent_row, "cfg", 0)
    noise_cond = jnp.where(branch == 0, kept_row, noise_pair)
    noise_uncond = jnp.where(branch == 0, noise_pair, kept_row)
    return noise_uncond + GUIDANCE * (noise_cond - noise_uncond)


def solution(mesh):
    in_specs = (
        P("cfg", "groups", ("blk", "ulysses"), None),
        P("cfg", "groups", ("blk", "ulysses"), None),
        P("cfg", "groups"),
        P("groups"),
        P(None, "groups", None),
        P(),
        P(None, ("blk", "ulysses", "cfg")),
        P(None, ("blk", "ulysses", "cfg")),
        P(None, None, ("ulysses", "cfg")),
        P(("ulysses", "cfg"), None),
        P("blk", ("ulysses", "cfg")),
        P(("ulysses", "cfg"), "blk"),
        P(),
        P(),
    )
    out_specs = P("groups", None, ("blk", "ulysses", "cfg"), None)


    return jax.shard_map(body, mesh=mesh, in_specs=in_specs, out_specs=out_specs, check_vma=False)
```

```python
import functools
import math

import jax
import jax.numpy as jnp
from jax import lax
from jax.experimental import pallas as pl
from jax.experimental.pallas import tpu as pltpu
from jax.sharding import PartitionSpec as P


GUIDANCE = 3.5
LN_EPS = 1e-06
RMS_EPS = 1e-06
NEG_FILL = -1e30
MESH = pl.DeviceIdType.MESH


def from_partner(value, axis, stride):
    mask = 2**stride
    pairs = [(source, source ^ mask) for source in range(lax.axis_size(axis))]
    return lax.ppermute(value, axis, pairs)


def sinusoid(timestep, feature_count):
    half_width = feature_count // 2
    frequency = jnp.exp(-math.log(10000.0) * jnp.arange(half_width, dtype=jnp.float32) / half_width)
    angles = timestep.astype(jnp.float32)[:, None] * frequency[None, :]
    return jnp.concatenate([jnp.cos(angles), jnp.sin(angles)], axis=1)


def layer_norm(values):
    average = jnp.mean(values, axis=-1, keepdims=True)
    centred = values - average
    variance = jnp.mean(centred * centred, axis=-1, keepdims=True)
    return centred * lax.rsqrt(variance + LN_EPS)


def modulate(values, shift, scale):
    return (layer_norm(values.astype(jnp.float32)) * (1.0 + scale) + shift).astype(jnp.bfloat16)


def rms_heads(values, gain):
    head_size = gain.shape[0]
    width = values.shape[-1]
    head_of = jnp.arange(width, dtype=jnp.int32) // head_size
    same_head = (head_of[:, None] == head_of[None, :]).astype(jnp.float32) / head_size
    mean_square = jnp.dot(
        values * values,
        same_head,
        precision=lax.Precision.HIGHEST,
        preferred_element_type=jnp.float32,
    )
    gains = jnp.tile(gain, width // head_size)
    return (values * lax.rsqrt(mean_square + RMS_EPS) * gains).astype(jnp.bfloat16)


def attention_kernel(head_size, q_ref, kv_ref, allowed_ref, o_ref):
    sides, batch, rows, width = q_ref.shape
    blocks, _, _, span, _ = kv_ref.shape
    lanes = 2 * head_size
    scale = 1.0 / math.sqrt(head_size)
    low = lax.broadcasted_iota(jnp.int32, (1, lanes), 1) < head_size
    for item in range(batch):
        allowed = allowed_ref[item] > 0.0
        for first in range(0, width, lanes):
            here = slice(first, first + lanes)
            queries = q_ref[:, item, :, here].reshape(sides * rows, lanes)
            keys = kv_ref[:, 0, item, :, here].reshape(blocks * span, lanes)
            values = kv_ref[:, 1, item, :, here].reshape(blocks * span, lanes)
            mixed = []
            for chosen in (low, jnp.logical_not(low)):
                one_head = jnp.where(chosen, queries, jnp.zeros_like(queries))
                scores = (
                    lax.dot_general(
                        one_head,
                        keys,
                        (((1,), (1,)), ((), ())),
                        preferred_element_type=jnp.float32,
                    )
                    * scale
                )
                scores = jnp.where(allowed, scores, NEG_FILL)
                largest = jnp.max(scores, axis=1, keepdims=True)
                weights = jnp.where(allowed, jnp.exp(scores - largest), 0.0)
                denominator = jnp.sum(weights, axis=1, keepdims=True)
                update = jnp.dot(
                    weights.astype(jnp.bfloat16), values, preferred_element_type=jnp.float32
                )
                mixed.append(update / denominator)
            both = jnp.where(low, mixed[0], mixed[1]).astype(jnp.bfloat16)
            o_ref[:, item, :, here] = both.reshape(sides, rows, lanes)


def attention(queries, all_kv, allowed, head_size):
    sides, batch, rows, width = queries.shape
    keys = all_kv.shape[0] * all_kv.shape[3]
    products = batch * sides * rows * keys * width
    return pl.pallas_call(
        functools.partial(attention_kernel, head_size),
        out_shape=jax.ShapeDtypeStruct(queries.shape, jnp.bfloat16),
        in_specs=[pl.BlockSpec(memory_space=pltpu.VMEM)] * 3,
        out_specs=pl.BlockSpec(memory_space=pltpu.VMEM),
        cost_estimate=pl.CostEstimate(
            flops=8 * products,
            bytes_accessed=4 * batch * keys * width + 4 * batch * sides * rows * width,
            transcendentals=products // head_size,
        ),
        name="attention",
    )(queries, all_kv, allowed)


def reduce_kernel(axes, x_ref, o_ref, got, mine, core_s, core_r, far_s, far_r):
    count = count_of(axes)
    me = flat_position(axes)
    core = lax.axis_index("cfg")
    partner = {"cfg": 1 - core}
    inner = x_ref.shape[2]
    barrier = pltpu.get_barrier_semaphore()
    pl.semaphore_signal(barrier, inc=1, device_id=partner, device_id_type=MESH)

    def target(step):
        return lax.rem(me + step, count)

    def greet(step, carry):
        pl.semaphore_signal(
            barrier, inc=1, device_id=coordinates(target(step), axes), device_id_type=MESH
        )
        return carry

    lax.fori_loop(1, count, greet, 0)
    pl.semaphore_wait(barrier, count)

    def beside(step):
        slot = target(step)
        return pltpu.make_async_remote_copy(
            src_ref=x_ref.at[slot // inner, 1 - core, lax.rem(slot, inner)],
            dst_ref=got.at[slot],
            send_sem=core_s.at[slot],
            recv_sem=core_r.at[slot],
            device_id=partner,
            device_id_type=MESH,
        )

    def far(step):
        slot = target(step)
        return pltpu.make_async_remote_copy(
            src_ref=mine.at[slot],
            dst_ref=o_ref.at[me],
            send_sem=far_s.at[step],
            recv_sem=far_r.at[step],
            device_id=coordinates(slot, axes),
            device_id_type=MESH,
        )

    def far_in(step):
        source = lax.rem(me - step + count, count)
        return pltpu.make_async_remote_copy(
            src_ref=mine.at[source],
            dst_ref=o_ref.at[source],
            send_sem=far_s.at[step],
            recv_sem=far_r.at[step],
            device_id=coordinates(source, axes),
            device_id_type=MESH,
        )

    def total(slot):
        own = x_ref[slot // inner, core, lax.rem(slot, inner)]
        beside_sum = own.astype(jnp.float32) + got[slot].astype(jnp.float32)
        return beside_sum.astype(jnp.bfloat16)

    def begin(step, carry):
        beside(step).start()
        return carry

    def send(step, carry):
        beside(step).wait_recv()
        mine[target(step)] = total(target(step))
        far(step).start()
        return carry

    def finish(step, carry):
        far_in(step).wait_recv()
        far(step).wait_send()
        beside(step).wait_send()
        return carry

    lax.fori_loop(1, count + 1, begin, 0)
    lax.fori_loop(1, count, send, 0)
    beside(0).wait_recv()
    o_ref[me] = total(me)
    lax.fori_loop(1, count, finish, 0)
    beside(0).wait_send()


def reduce_cores(value, axes, collective_id):
    count = value.shape[0] * value.shape[2]
    shape = (count,) + value.shape[3:]
    sems = pltpu.SemaphoreType.DMA((count,))
    return pl.pallas_call(
        functools.partial(reduce_kernel, axes),
        out_shape=jax.ShapeDtypeStruct(shape, value.dtype),
        in_specs=[pl.BlockSpec(memory_space=pltpu.VMEM)],
        out_specs=pl.BlockSpec(memory_space=pltpu.VMEM),
        scratch_shapes=[
            pltpu.VMEM(shape, value.dtype),
            pltpu.VMEM(shape, value.dtype),
            sems,
            sems,
            sems,
            sems,
        ],
        compiler_params=pltpu.CompilerParams(collective_id=collective_id, has_side_effects=True),
        cost_estimate=pl.CostEstimate(
            flops=0, bytes_accessed=8 * math.prod(shape) + 4000000, transcendentals=0
        ),
    )(value)


def flat_position(axes):
    position = 0
    for axis in axes:
        position = position * lax.axis_size(axis) + lax.axis_index(axis)
    return position


def coordinates(position, axes):
    found = {}
    for axis in reversed(axes):
        size = lax.axis_size(axis)
        found[axis] = lax.rem(position, size)
        position = position // size
    return found


def count_of(axes):
    return math.prod(lax.axis_size(axis) for axis in axes)


def direct_kernel(axes, swap, x_ref, o_ref, send_sem, recv_sem, local_sem):
    count = count_of(axes)
    me = flat_position(axes)
    barrier = pltpu.get_barrier_semaphore()

    def greet(step, carry):
        peer = lax.rem(me + step, count)
        pl.semaphore_signal(
            barrier, inc=1, device_id=coordinates(peer, axes), device_id_type=MESH
        )
        return carry

    lax.fori_loop(1, count, greet, 0)
    own = pltpu.make_async_copy(x_ref.at[me] if swap else x_ref, o_ref.at[me], local_sem)
    own.start()
    pl.semaphore_wait(barrier, count - 1)

    def outgoing(step):
        peer = lax.rem(me + step, count)
        return pltpu.make_async_remote_copy(
            src_ref=x_ref.at[peer] if swap else x_ref,
            dst_ref=o_ref.at[me],
            send_sem=send_sem.at[step],
            recv_sem=recv_sem.at[step],
            device_id=coordinates(peer, axes),
            device_id_type=MESH,
        )

    def incoming(step):
        source = lax.rem(me - step + count, count)
        return pltpu.make_async_remote_copy(
            src_ref=x_ref.at[source] if swap else x_ref,
            dst_ref=o_ref.at[source],
            send_sem=send_sem.at[step],
            recv_sem=recv_sem.at[step],
            device_id=coordinates(source, axes),
            device_id_type=MESH,
        )

    def begin(step, carry):
        outgoing(step).start()
        return carry

    def finish(step, carry):
        incoming(step).wait_recv()
        outgoing(step).wait_send()
        return carry

    lax.fori_loop(1, count, begin, 0)
    lax.fori_loop(1, count, finish, 0)
    own.wait()


def direct(value, axes, swap, collective_id):
    count = count_of(axes)
    shape = value.shape if swap else (count,) + value.shape
    return pl.pallas_call(
        functools.partial(direct_kernel, axes, swap),
        out_shape=jax.ShapeDtypeStruct(shape, value.dtype),
        in_specs=[pl.BlockSpec(memory_space=pltpu.VMEM)],
        out_specs=pl.BlockSpec(memory_space=pltpu.VMEM),
        scratch_shapes=[
            pltpu.SemaphoreType.DMA((count,)),
            pltpu.SemaphoreType.DMA((count,)),
            pltpu.SemaphoreType.DMA,
        ],
        compiler_params=pltpu.CompilerParams(collective_id=collective_id, has_side_effects=True),
        cost_estimate=pl.CostEstimate(
            flops=0, bytes_accessed=4 * math.prod(shape) + 4000000, transcendentals=0
        ),
    )(value)


def quad_kernel(
    chunks, x_ref, o_ref, send_u, recv_u, send_c, recv_c, send_f, recv_f, local_sem
):
    size = lax.axis_size("ulysses")
    row = lax.axis_index("ulysses")
    core = lax.axis_index("cfg")
    me = row * 2 + core
    partner = {"ulysses": row, "cfg": 1 - core}
    barrier = pltpu.get_barrier_semaphore()
    for step in range(1, size):
        pl.semaphore_signal(
            barrier,
            inc=1,
            device_id={"ulysses": lax.rem(row + step, size), "cfg": core},
            device_id_type=MESH,
        )
    pl.semaphore_signal(barrier, inc=1, device_id=partner, device_id_type=MESH)
    own = pltpu.make_async_copy(x_ref, o_ref.at[me], local_sem)
    own.start()
    pl.semaphore_wait(barrier, size)

    def across(step, chunk):
        return pltpu.make_async_remote_copy(
            src_ref=x_ref.at[chunk],
            dst_ref=o_ref.at[me, chunk],
            send_sem=send_u.at[step, chunk],
            recv_sem=recv_u.at[step, chunk],
            device_id={"ulysses": lax.rem(row + step, size), "cfg": core},
            device_id_type=MESH,
        )

    def landed(step, chunk):
        source = lax.rem(row - step + size, size)
        return pltpu.make_async_remote_copy(
            src_ref=x_ref.at[chunk],
            dst_ref=o_ref.at[source * 2 + core, chunk],
            send_sem=send_u.at[step, chunk],
            recv_sem=recv_u.at[step, chunk],
            device_id={"ulysses": source, "cfg": core},
            device_id_type=MESH,
        )

    def forward(step, chunk, side):
        source = lax.rem(row - step + size, size)
        return pltpu.make_async_remote_copy(
            src_ref=o_ref.at[source * 2 + side, chunk],
            dst_ref=o_ref.at[source * 2 + side, chunk],
            send_sem=send_f.at[step, chunk],
            recv_sem=recv_f.at[step, chunk],
            device_id=partner,
            device_id_type=MESH,
        )

    def beside(slot):
        return pltpu.make_async_remote_copy(
            src_ref=x_ref,
            dst_ref=o_ref.at[slot],
            send_sem=send_c,
            recv_sem=recv_c,
            device_id=partner,
            device_id_type=MESH,
        )

    pairs = [(step, chunk) for chunk in range(chunks) for step in range(1, size)]
    for step, chunk in pairs:
        across(step, chunk).start()
    beside(me).start()
    for step, chunk in pairs:
        landed(step, chunk).wait_recv()
        forward(step, chunk, core).start()
    for step, chunk in pairs:
        across(step, chunk).wait_send()
        forward(step, chunk, core).wait_send()
        forward(step, chunk, 1 - core).wait_recv()
    beside(me).wait_send()
    beside(row * 2 + 1 - core).wait_recv()
    own.wait()


def quad_gather(value, collective_id):
    size = lax.axis_size("ulysses")
    chunks = value.shape[0]
    shape = (size * 2,) + value.shape
    grid_sem = pltpu.SemaphoreType.DMA((size, chunks))
    return pl.pallas_call(
        functools.partial(quad_kernel, chunks),
        out_shape=jax.ShapeDtypeStruct(shape, value.dtype),
        in_specs=[pl.BlockSpec(memory_space=pl.ANY)],
        out_specs=pl.BlockSpec(memory_space=pl.ANY),
        scratch_shapes=[
            grid_sem,
            grid_sem,
            pltpu.SemaphoreType.DMA,
            pltpu.SemaphoreType.DMA,
            grid_sem,
            grid_sem,
            pltpu.SemaphoreType.DMA,
        ],
        compiler_params=pltpu.CompilerParams(collective_id=collective_id, has_side_effects=True),
        cost_estimate=pl.CostEstimate(
            flops=0, bytes_accessed=8 * math.prod(shape) + 4000000, transcendentals=0
        ),
    )(value)


def ring_kernel(axis, spread, x_ref, o_ref, hop_s, hop_r, x_s, x_r, c_s, c_r, f_s, f_r, local_sem):
    size = lax.axis_size(axis)
    me = lax.axis_index(axis)
    last = size // 2
    halved = size % 2 == 0
    sides = lax.axis_size("ulysses") if spread else 1
    row = lax.axis_index("ulysses")
    core = lax.axis_index("cfg")
    partner = {"ulysses": row, "cfg": 1 - core}
    base = o_ref.at[row * 2 + core] if spread else o_ref

    def at(offset):
        return lax.rem(me + offset + size, size)

    def aside(step):
        return {"ulysses": lax.rem(row + step, sides), "cfg": core}

    barrier = pltpu.get_barrier_semaphore()
    for way in (1, -1):
        pl.semaphore_signal(barrier, inc=1, device_id={axis: at(way)}, device_id_type=MESH)
    if spread:
        for step in range(1, sides):
            pl.semaphore_signal(barrier, inc=1, device_id=aside(step), device_id_type=MESH)
        pl.semaphore_signal(barrier, inc=1, device_id=partner, device_id_type=MESH)
    own = pltpu.make_async_copy(x_ref, base.at[me], local_sem)
    own.start()
    pl.semaphore_wait(barrier, 2 + (sides if spread else 0))

    def part(ref, way, step):
        if halved and step == last:
            return ref.at[0 if way == 1 else 1]
        return ref

    def hop(way, step):
        slot = at(-way * (step - 1))
        source = x_ref if step == 1 else base.at[slot]
        return pltpu.make_async_remote_copy(
            src_ref=part(source, way, step),
            dst_ref=part(base.at[slot], way, step),
            send_sem=hop_s.at[(way + 1) // 2, step],
            recv_sem=hop_r.at[(way + 1) // 2, step],
            device_id={axis: at(way)},
            device_id_type=MESH,
        )

    def hop_in(way, step):
        slot = base.at[at(-way * step)]
        return pltpu.make_async_remote_copy(
            src_ref=part(slot, way, step),
            dst_ref=part(slot, way, step),
            send_sem=hop_s.at[(way + 1) // 2, step],
            recv_sem=hop_r.at[(way + 1) // 2, step],
            device_id={axis: at(-way)},
            device_id_type=MESH,
        )

    def send(order, offset, step):
        slot = at(offset)
        return pltpu.make_async_remote_copy(
            src_ref=x_ref if order == 0 else base.at[slot],
            dst_ref=base.at[slot],
            send_sem=x_s.at[order, step] if step else c_s.at[order],
            recv_sem=x_r.at[order, step] if step else c_r.at[order],
            device_id=aside(step) if step else partner,
            device_id_type=MESH,
        )

    def across_in(order, offset, step):
        source = lax.rem(row - step + sides, sides)
        block = o_ref.at[source * 2 + core, at(offset)]
        return pltpu.make_async_remote_copy(
            src_ref=block,
            dst_ref=block,
            send_sem=x_s.at[order, step],
            recv_sem=x_r.at[order, step],
            device_id=aside(step),
            device_id_type=MESH,
        )

    def forward(order, offset, step, side):
        source = lax.rem(row - step + sides, sides)
        block = o_ref.at[source * 2 + side, at(offset)]
        return pltpu.make_async_remote_copy(
            src_ref=block,
            dst_ref=block,
            send_sem=f_s.at[order, step],
            recv_sem=f_r.at[order, step],
            device_id=partner,
            device_id_type=MESH,
        )

    def beside_in(order, offset):
        block = o_ref.at[row * 2 + 1 - core, at(offset)]
        return pltpu.make_async_remote_copy(
            src_ref=block,
            dst_ref=block,
            send_sem=c_s.at[order],
            recv_sem=c_r.at[order],
            device_id=partner,
            device_id_type=MESH,
        )

    steps = last
    offsets = [0]
    for way in (1, -1):
        hop(way, 1).start()
    sent = []

    def pass_on(order, offset):
        if spread:
            for step in list(range(1, sides)) + [0]:
                send(order, offset, step).start()
            sent.append((order, offset))

    def relay(order, offset):
        for step in range(1, sides):
            across_in(order, offset, step).wait_recv()
            forward(order, offset, step, core).start()

    pass_on(0, 0)
    relayed = 0
    for step in range(1, steps + 1):
        final = halved and step == last
        for way in (1, -1):
            hop_in(way, step).wait_recv()
            if step < steps:
                hop(way, step + 1).start()
            if not final:
                offsets.append(-way * step)
                pass_on(len(offsets) - 1, offsets[-1])
        if final:
            offsets.append(step)
            pass_on(len(offsets) - 1, step)
        if spread:
            while relayed < len(offsets) - 2:
                relay(relayed, offsets[relayed])
                relayed += 1
    if spread:
        while relayed < len(offsets):
            relay(relayed, offsets[relayed])
            relayed += 1
    for step in range(1, steps + 1):
        for way in (1, -1):
            hop(way, step).wait_send()
    for order, offset in sent:
        for step in range(sides):
            send(order, offset, step).wait_send()
        for step in range(1, sides):
            forward(order, offset, step, core).wait_send()
            forward(order, offset, step, 1 - core).wait_recv()
        beside_in(order, offset).wait_recv()
    own.wait()


def ring_gather(value, axis, spread, collective_id):
    size = lax.axis_size(axis)
    sides = lax.axis_size("ulysses")
    shape = (size,) + value.shape
    if spread:
        shape = (sides * 2,) + shape
    space = pl.ANY if spread else pltpu.VMEM
    hops = pltpu.SemaphoreType.DMA((2, size // 2 + 1))
    across = pltpu.SemaphoreType.DMA((size, sides))
    beside = pltpu.SemaphoreType.DMA((size,))
    return pl.pallas_call(
        functools.partial(ring_kernel, axis, spread),
        out_shape=jax.ShapeDtypeStruct(shape, value.dtype),
        in_specs=[pl.BlockSpec(memory_space=space)],
        out_specs=pl.BlockSpec(memory_space=space),
        scratch_shapes=[hops, hops, across, across, beside, beside, across, across]
        + [pltpu.SemaphoreType.DMA],
        compiler_params=pltpu.CompilerParams(collective_id=collective_id, has_side_effects=True),
        cost_estimate=pl.CostEstimate(
            flops=0, bytes_accessed=8 * math.prod(shape) + 4000000, transcendentals=0
        ),
    )(value)


class WeightRing:
    def __init__(self, piece, axis, across):
        self.axis, self.across = axis, across
        self.size = lax.axis_size(axis)
        self.parts = lax.axis_size(across)
        self.me = lax.axis_index(axis)
        self.part = lax.axis_index(across)
        self.rows = piece.shape[0]
        self.share = self.rows // self.parts
        self.up = [(source, (source + 1) % self.size) for source in range(self.size)]
        self.down = [(source, (source - 1) % self.size) for source in range(self.size)]
        whole = jnp.zeros((self.size * self.rows,) + piece.shape[1:], piece.dtype)
        self.whole = lax.dynamic_update_slice_in_dim(whole, piece, self.me * self.rows, 0)
        own = lax.dynamic_slice_in_dim(piece, self.part * self.share, self.share, 0)
        self.upward = self.downward = own

    def place(self, block, owner, offset):
        for step in range(self.parts):
            if step:
                pairs = [(part, (part + step) % self.parts) for part in range(self.parts)]
                moved = lax.ppermute(block, self.across, pairs)
            else:
                moved = block
            origin = lax.rem(self.part - step + self.parts, self.parts)
            start = owner * self.rows + origin * self.share + offset
            self.whole = lax.dynamic_update_slice_in_dim(self.whole, moved, start, 0)

    def hop(self, step, after):
        size, me = self.size, self.me
        self.upward, self.downward, after = lax.optimization_barrier(
            (self.upward, self.downward, after)
        )
        if step <= (size - 1) // 2:
            self.upward = lax.ppermute(self.upward, self.axis, self.up)
            self.downward = lax.ppermute(self.downward, self.axis, self.down)
            self.place(self.upward, lax.rem(me - step + size, size), 0)
            self.place(self.downward, lax.rem(me + step, size), 0)
        else:
            half = self.share // 2
            far = lax.rem(me + step, size)
            low = lax.ppermute(self.upward[:half], self.axis, self.up)
            high = lax.ppermute(self.downward[half:], self.axis, self.down)
            self.place(jnp.concatenate([low, high], axis=0), far, 0)
        return after


def body(
    img_tokens,
    text_tokens,
    text_lengths,
    timestep,
    pooled,
    time_weight,
    time_second,
    mod_weight,
    proj_weight,
    out_weight,
    expand_weight,
    reduce_weight,
    qk_gain,
    final_weight,
):
    model_width = img_tokens.shape[3]
    prompts = img_tokens.shape[1]
    branches = pooled.shape[0]
    branch = lax.axis_index("cfg")
    everyone = ("blk", "ulysses", "cfg")
    blocks = lax.axis_size("blk")
    sides = lax.axis_size("ulysses")
    ring = WeightRing(expand_weight, "blk", "groups")
    sinusoid_rows = sinusoid(timestep, time_weight.shape[0]).astype(jnp.bfloat16)
    time_hidden = jax.nn.silu(
        jnp.dot(sinusoid_rows, time_weight, preferred_element_type=jnp.float32)
    ).astype(jnp.bfloat16)
    time_part = jnp.dot(time_hidden, time_second, preferred_element_type=jnp.float32)
    time_width = time_part.shape[1]
    first = direct(
        jnp.concatenate([time_part, text_lengths[0][:, None].astype(jnp.float32)], axis=1),
        everyone,
        False,
        0,
    )
    time_embed = first[:, :, :time_width].transpose(1, 0, 2).reshape(prompts, -1)
    lengths = first[:branches, :, time_width].astype(jnp.int32)
    acted = jax.nn.silu(time_embed[None] + pooled).astype(jnp.bfloat16)
    mod_part = jnp.einsum("bpd,dc->bpc", acted, mod_weight, preferred_element_type=jnp.float32)
    mod_all = direct(mod_part, everyone, False, 1)
    mod_all = ring.hop(1, mod_all)
    own_mod = lax.dynamic_index_in_dim(mod_all, branch, 1, keepdims=False)
    own_mod = own_mod.transpose(1, 0, 2).reshape(prompts, 10, model_width)
    image_rows = img_tokens[0]
    text_rows = text_tokens[0]
    token_count = image_rows.shape[1]
    slot_count = text_rows.shape[1]
    h_img = modulate(image_rows, own_mod[:, 0:1], own_mod[:, 1:2])
    h_txt = modulate(text_rows, own_mod[:, 4:5], own_mod[:, 3:4])
    rows_own = jnp.concatenate([h_img, h_txt], axis=1)
    rows_all = quad_gather(rows_own, 2)
    rows_all = rows_all.reshape(sides, branches, prompts, token_count + slot_count, model_width)
    rows_img = rows_all[:, :, :, :token_count]
    rows_txt = rows_all[:, :, :, token_count:]
    img_proj = jnp.einsum(
        "ubprd,jdc->jubprc", rows_img, proj_weight[0:3], preferred_element_type=jnp.float32
    )
    txt_proj = jnp.einsum(
        "ubprd,jdc->jubprc", rows_txt, proj_weight[3:5], preferred_element_type=jnp.float32
    )
    batch = branches * prompts
    inner_local = img_proj.shape[-1]
    queries = rms_heads(img_proj[0], qk_gain[0]).reshape(sides, batch, token_count, inner_local)

    def by_item(keys, values):
        pair = jnp.stack([keys, values]).reshape(2, sides, batch, -1, inner_local)
        return pair.transpose(0, 2, 1, 3, 4).reshape(2, batch, -1, inner_local)

    img_kv = by_item(rms_heads(img_proj[1], qk_gain[1]), img_proj[2].astype(jnp.bfloat16))
    txt_kv = by_item(rms_heads(txt_proj[0], qk_gain[2]), txt_proj[1].astype(jnp.bfloat16))
    img_span = img_kv.shape[2]
    txt_span = txt_kv.shape[2]
    padding = -txt_span % 16
    own_kv = jnp.concatenate(
        [img_kv, jnp.pad(txt_kv, ((0, 0), (0, 0), (0, padding), (0, 0)))], axis=2
    )
    all_kv = ring_gather(own_kv, "blk", False, 6)
    for step in range(2, blocks // 2 + 1):
        all_kv = ring.hop(step, all_kv)
    place = jnp.arange(img_span + txt_span + padding, dtype=jnp.int32) - img_span
    slot = jnp.arange(blocks, dtype=jnp.int32)[:, None] * txt_span + place
    live = (slot < lengths.reshape(batch, 1, 1)) & (place < txt_span)
    allowed = ((place < 0) | live).astype(jnp.float32).reshape(batch, 1, -1)
    mixed = attention(queries, all_kv, allowed, qk_gain.shape[1])
    out_terms = jnp.dot(
        mixed.reshape(-1, inner_local), out_weight, preferred_element_type=jnp.float32
    )
    out_terms = out_terms.astype(jnp.bfloat16).reshape(
        sides, branches, 1, prompts * token_count, model_width
    )
    out_terms = reduce_cores(out_terms, ("ulysses",), 3)
    attended = jnp.sum(out_terms.astype(jnp.float32), axis=0)
    attended = attended.reshape(prompts, token_count, model_width)
    residual = image_rows.astype(jnp.float32) + own_mod[:, 2:3] * attended
    feed_input = modulate(residual, own_mod[:, 7:8], own_mod[:, 8:9]).reshape(
        prompts * token_count, model_width
    )
    feed_halves = feed_input.reshape(2, -1, model_width)
    feed_all = ring_gather(feed_halves, "blk", True, 4)
    feed_all = feed_all.reshape(-1, model_width)
    pre_active = jnp.dot(feed_all, ring.whole, preferred_element_type=jnp.float32)
    feed_hidden = jax.nn.gelu(pre_active, approximate=True).astype(jnp.bfloat16)
    feed_hidden = lax.optimization_barrier(feed_hidden)
    feed_terms = jnp.dot(feed_hidden, reduce_weight, preferred_element_type=jnp.float32)
    feed_terms = feed_terms.astype(jnp.bfloat16).reshape(
        sides, branches, blocks, prompts * token_count, -1
    )
    feed_terms = reduce_cores(feed_terms, ("ulysses", "blk"), 5)
    feed_terms = feed_terms.reshape(sides, blocks, prompts * token_count, -1)
    feed_out = jnp.sum(feed_terms.astype(jnp.float32), axis=0).transpose(1, 0, 2)
    second_residual = residual + own_mod[:, 9:10] * feed_out.reshape(
        prompts, token_count, model_width
    )
    final_rows = modulate(second_residual, own_mod[:, 6:7], own_mod[:, 5:6])
    noise = jnp.einsum("prd,dc->prc", final_rows, final_weight, preferred_element_type=jnp.float32)
    latent_channels = final_weight.shape[1] // 4
    noise_own = noise.reshape(prompts, token_count, 2, 2, latent_channels).transpose(0, 4, 2, 1, 3)
    noise_own = noise_own.reshape(prompts, latent_channels, 2, 2 * token_count)
    kept_row = lax.dynamic_slice_in_dim(noise_own, branch, 1, 2)
    sent_row = lax.dynamic_slice_in_dim(noise_own, 1 - branch, 1, 2)
    noise_pair = from_partner(sent_row, "cfg", 0)
    noise_cond = jnp.where(branch == 0, kept_row, noise_pair)
    noise_uncond = jnp.where(branch == 0, noise_pair, kept_row)
    return noise_uncond + GUIDANCE * (noise_cond - noise_uncond)


def solution(mesh):
    in_specs = (
        P("cfg", "groups", ("blk", "ulysses"), None),
        P("cfg", "groups", ("blk", "ulysses"), None),
        P("cfg", "groups"),
        P("groups"),
        P(None, "groups", None),
        P(),
        P(None, ("blk", "ulysses", "cfg")),
        P(None, ("blk", "ulysses", "cfg")),
        P(None, None, ("ulysses", "cfg")),
        P(("ulysses", "cfg"), None),
        P("blk", ("ulysses", "cfg")),
        P(("ulysses", "cfg"), "blk"),
        P(),
        P(),
    )
    out_specs = P("groups", None, ("blk", "ulysses", "cfg"), None)


    return jax.shard_map(body, mesh=mesh, in_specs=in_specs, out_specs=out_specs, check_vma=False)
```
